32 devices in a mesh: wide: 8 (over y, x, core), narrow: 4 (over z).
Axes of the slice: x: 2, y: 2, z: 4, core: 2. Of those that a mesh axis runs over, the one named last changes fastest.
Arguments:
- feat_queries: bfloat16 [8192, 256], P(('wide', 'narrow')), may hold values from -6 to 6
- feat_keys: bfloat16 [8192, 256], P(('wide', 'narrow')), may hold values from -6 to 6
- values: bfloat16 [8192, 1024], P(('wide', 'narrow')), may hold values from -8 to 8
- window_queries: bfloat16 [8192, 1024], P(('wide', 'narrow')), may hold values from -150 to 150
- window_keys: bfloat16 [8192, 1024], P(('wide', 'narrow')), may hold values from -5 to 5
Outputs:
- mixed: bfloat16 [8192, 1024], P(('wide', 'narrow'))
The draws below stay inside these ranges and needn't reach their ends.
All inputs are finite; a program needn't handle non-finite values.
Results may differ from the reference program's by a relative error of at most 0.0004.
The reference program's roundings to bfloat16 on the way (of `a` and `probs`) count: a program that leaves them out, or rounds other values in their place, can miss the bound.
Values may be sent and summed in bfloat16 or wider, within the bound.
A program may use at most 64 MiB of HBM per device.

```python
import jax
import jax.numpy as jnp
import numpy as np
from jax import lax

HEADS = 16
FEAT_DIM = 16
VDIM = 64
WHEAD = 64
WINDOW = 256
TOK_DEV = 256
SEQ = 8192


def shared_keys(key):
    return jnp.clip(jax.random.normal(jax.random.fold_in(key, 71), (SEQ, HEADS * WHEAD), jnp.float32), -5.0, 5.0)


def draw_window_keys(key, part):
    return shared_keys(key).astype(jnp.bfloat16)


def draw_window_queries(key, part):
    base = jnp.clip(jax.random.normal(jax.random.fold_in(key, 83), (SEQ, HEADS * WHEAD), jnp.float32), -5.0, 5.0)
    return base.astype(jnp.bfloat16)


def draw_values(key, part):
    channels = HEADS * VDIM
    steps = jax.random.normal(jax.random.fold_in(key, 131), (SEQ, channels), jnp.float32) * jnp.float32((1.0 / SEQ) ** 0.5)
    drift = jnp.cumsum(steps, 0)
    offset = jax.random.uniform(jax.random.fold_in(key, 137), (1, channels), jnp.float32, -1.0, 1.0)
    rough = jnp.clip(jax.random.normal(jax.random.fold_in(key, 139), (SEQ, channels), jnp.float32), -4.0, 4.0)
    level = offset + drift
    return jnp.clip(rough + level, -8.0, 8.0).astype(jnp.bfloat16)


def steps_of(stream_key, dims, pieces, low, high):
    loudness, own = 1.0, jax.random.fold_in(stream_key, 6)
    for axis_at, shards_of in pieces:
        steps = jnp.exp(jax.random.uniform(jax.random.fold_in(own, axis_at), (shards_of,), jnp.float32, low / len(pieces), high / len(pieces)))
        loudness = loudness * jnp.repeat(steps, dims[axis_at] // shards_of).reshape([-1 if axis == axis_at else 1 for axis in range(len(dims))])
    return loudness


def centred(rng, extent, scale, reach, pieces=(), kind=jnp.bfloat16):
    drawn = jax.random.normal(rng, extent, jnp.float32) * scale
    if len(pieces) > 0:
        drawn = steps_of(rng, extent, pieces, -0.22, 0.18) * drawn
    return jnp.clip(drawn, min=-reach, max=reach).astype(kind)


def setup_inputs(seed: int = 0) -> dict:
    key_of = jax.random.split(jax.random.key(seed), 6)
    return {
        "feat_queries": centred(key_of[0], (SEQ, HEADS * FEAT_DIM), 1.0, 6.0, ((0, 32),)),
        "feat_keys": centred(key_of[1], (SEQ, HEADS * FEAT_DIM), 1.0, 6.0, ((0, 32),)),
        "values": draw_values(jax.random.fold_in(key_of[5], 71), 0),
        "window_queries": draw_window_queries(jax.random.fold_in(key_of[5], 71), 0),
        "window_keys": draw_window_keys(jax.random.fold_in(key_of[5], 71), 0),
    }


def expand(x, heads):
    rows = x.shape[0]
    x = x.astype(jnp.float32).reshape(rows, heads, -1)
    width = x.shape[-1]
    first, second = np.triu_indices(width)
    weight = np.where(first == second, 1.0 / np.sqrt(2.0 * width), 1.0 / np.sqrt(1.0 * width))
    quad = x[..., first] * x[..., second] * jnp.asarray(weight, jnp.float32)
    ones = jnp.ones((rows, heads, 1), jnp.float32)
    return jnp.concatenate([ones, x / width ** 0.25, quad], -1).astype(jnp.bfloat16)

def layer_block(qf, kf, values, wq, wk, rim_keys, rim_values, start, prior_state, prior_norm):
    rows, heads, feats = qf.shape
    val3 = values.reshape(rows, heads, -1)
    scores = jnp.einsum('thf,shf->hts', qf, kf, preferred_element_type=jnp.float32)
    causal = lax.broadcasted_iota(jnp.int32, (rows, rows), 0) >= lax.broadcasted_iota(jnp.int32, (rows, rows), 1)
    scores = jnp.where(causal[None], scores, jnp.float32(0.0))
    intra_den = lax.optimization_barrier(jnp.sum(scores, -1))
    intra_num = jnp.einsum('hts,shv->thv', scores.astype(jnp.bfloat16), val3, preferred_element_type=jnp.float32)
    qwide = qf.astype(jnp.float32)
    cross_num = jnp.einsum('thf,fhv->thv', qwide, prior_state.reshape(feats, heads, -1), precision=lax.Precision.HIGHEST)
    cross_den = jnp.einsum('thf,fh->th', qwide, prior_norm, precision=lax.Precision.HIGHEST)
    linear = (intra_num + cross_num) / (intra_den.T + cross_den)[..., None]
    span = rim_keys.shape[0]
    keys3 = jnp.concatenate([rim_keys, wk], 0).reshape(span + rows, heads, -1)
    vals3 = jnp.concatenate([rim_values, values], 0).reshape(span + rows, heads, -1)
    query3 = wq.reshape(rows, heads, -1)
    logits = jnp.einsum('thd,shd->hts', query3, keys3, preferred_element_type=jnp.float32) / jnp.sqrt(jnp.float32(query3.shape[-1]))
    row = lax.broadcasted_iota(jnp.int32, (rows, span + rows), 0)
    col = lax.broadcasted_iota(jnp.int32, (rows, span + rows), 1)
    valid = (col > row) & (col <= row + span) & (col - span + start >= 0)
    logits = jnp.where(valid[None], logits, jnp.float32(-1e+30))
    peak = lax.optimization_barrier(jnp.max(logits, -1, keepdims=True))
    expo = jnp.where(valid[None], jnp.exp(logits - peak), jnp.float32(0.0))
    probs = (expo / lax.optimization_barrier(jnp.sum(expo, -1, keepdims=True))).astype(jnp.bfloat16)
    window = jnp.einsum('hts,shv->thv', probs, vals3, preferred_element_type=jnp.float32)
    mixed = (linear + window).reshape(rows, -1).astype(jnp.bfloat16)
    own_state = jnp.einsum('shf,shv->fhv', kf, val3, preferred_element_type=jnp.float32).reshape(feats, -1)
    own_norm = lax.optimization_barrier(jnp.sum(kf.astype(jnp.float32), 0)).T
    return (mixed, own_state, own_norm)

def reference(feat_queries, feat_keys, values, window_queries, window_keys):
    blocks = SEQ // TOK_DEV
    span = WINDOW

    def split(a):
        return a.reshape(blocks, TOK_DEV, a.shape[-1])

    def step(carry, inputs):
        state, norm, rim_keys, rim_values = carry
        index, fq, fk, vv, wq, wk = inputs
        qf = expand(fq, HEADS)
        kf = expand(fk, HEADS)
        start = (index * TOK_DEV).astype(jnp.int32)
        mixed, own_state, own_norm = layer_block(qf, kf, vv, wq, wk, rim_keys, rim_values, start, state, norm)
        carry = (state + own_state, norm + own_norm, wk[TOK_DEV - span:], vv[TOK_DEV - span:])
        return (carry, mixed)
    feats = 1 + FEAT_DIM + FEAT_DIM * (FEAT_DIM + 1) // 2
    init = (jnp.zeros((feats, HEADS * VDIM), jnp.float32), jnp.zeros((feats, HEADS), jnp.float32), jnp.zeros((span, HEADS * WHEAD), jnp.bfloat16), jnp.zeros((span, HEADS * VDIM), jnp.bfloat16))
    xs = (jnp.arange(blocks, dtype=jnp.int32), split(feat_queries), split(feat_keys), split(values), split(window_queries), split(window_keys))
    carry, mixed = lax.scan(step, init, xs)
    return mixed.reshape(SEQ, HEADS * VDIM)
```

```python
import functools

import jax
import jax.numpy as jnp
import numpy as np
from jax import lax
from jax.experimental import pallas as pl
from jax.experimental.pallas import tpu as pltpu
from jax.sharding import PartitionSpec as P

HEADS = 16
WINDOW = 256
LANES = 128
EARLY = 3
MORE = 1
AHEAD = 4
GROUP = 4
FAR = 6
PACE = 13
MIX = 2
RATE = 1
LAG = 2
FINE = 65000.0
MESH = pl.DeviceIdType.MESH
F32 = jnp.float32
BF16 = jnp.bfloat16
NT = (((1,), (1,)), ((), ()))


def nt(a, b):
    return lax.dot_general(a, b, NT, preferred_element_type=F32)


def nn(a, b):
    return jnp.dot(a, b, preferred_element_type=F32)


def layout(width):
    norms = 1 + 2 * width
    return norms, -(-(norms + 5) // 8) * 8


def tables(width):
    norms, plain = layout(width)
    pairs = [(i, i) for i in range(width)] + [(i, j) for i in range(width) for j in range(i + 1, width)]
    padded = plain + -(-(len(pairs) - width) // 24) * 24
    per = LANES // width
    one = np.zeros((padded, width))
    two = np.zeros((padded, width))
    extra = np.zeros((8, padded))
    extra[0, 0] = 1.0
    extra[1, : 1 + width] = 1.0
    extra[2, 0] = 1.0
    extra[2, 1 : 1 + width] = 1.0 / width**0.25
    for i in range(width):
        one[1 + i, i] = 1.0
    for n, (i, j) in enumerate(pairs):
        at = 1 + width + n if n < width else plain + n - width
        one[at, i] = 1.0
        two[at, j] = 1.0
        extra[2, at] = 1.0 / np.sqrt(2.0 * width) if i == j else 1.0 / np.sqrt(1.0 * width)
    pick = np.zeros((2, per, padded, LANES))
    for j in range(per):
        pick[0, j, :, j * width : (j + 1) * width] = one
        pick[1, j, :, j * width : (j + 1) * width] = two
    return padded, per, pick, extra


def kernel(
    dims,
    fq_in, fk_in, val_in, wq_in, wk_in, pick_in, crow_in, ccol_in,
    out,
    fq, fk, val, wq, wk, pick, crow, ccol,
    qf, kft, state, got, upin, upout, downin, downout, scan, prior, rimk, rimv, num, den, held,
    load, send1, recv1, send2, recv2, usend, urecv, dsend, drecv, rsend, rrecv,
):
    wide, narrow, padded, per, share = dims
    NORMS, PLAIN = layout(fq_in.shape[1] // HEADS)
    n = wide * narrow
    rows = val.shape[0]
    pairs = val.shape[1] // LANES
    chop = padded // share
    mw = lax.axis_index("wide")
    mz = lax.axis_index("narrow")
    me = mw * narrow + mz
    top_z = mz == narrow - 1
    not_last = me < n - 1

    ins = (fk_in, pick_in, ccol_in, val_in, fq_in, crow_in, wq_in, wk_in)
    mine = (fk, pick, ccol, val, fq, crow, wq, wk)
    loads = [pltpu.make_async_copy(i, m, load.at[j]) for j, (i, m) in enumerate(zip(ins, mine))]
    for one in loads:
        one.start()

    def where_is(d):
        return {"wide": lax.div(d, narrow), "narrow": lax.rem(d, narrow)}

    def other(k):
        return lax.rem(mw + k, wide)

    barrier = pltpu.get_barrier_semaphore()

    def greet(d):
        pl.semaphore_signal(barrier, inc=1, device_id=d, device_id_type=MESH)

    @pl.loop(1, wide)
    def _(k):
        greet({"wide": other(k), "narrow": mz})

    @pl.when(jnp.logical_not(top_z))
    def _():
        greet({"wide": mw, "narrow": mz + 1})

    @pl.when(mz > 0)
    def _():
        greet({"wide": mw, "narrow": mz - 1})

    @pl.when(top_z & not_last)
    def _():
        greet(where_is(me + 1))

    @pl.when((mz == 0) & (me > 0))
    def _():
        greet(where_is(me - 1))

    @pl.when(mz == 0)
    def _():
        upin[...] = jnp.zeros_like(upin)

    @pl.when(top_z)
    def _():
        downin[...] = jnp.zeros_like(downin)

    downin[pl.ds(0, upin.shape[0] // wide), :] = jnp.zeros((upin.shape[0] // wide, LANES), F32)

    @pl.when(me == 0)
    def _():
        rimk[...] = jnp.zeros_like(rimk)
        rimv[...] = jnp.zeros_like(rimv)

    def cols(p):
        return pl.ds(pl.multiple_of(p * LANES, LANES), LANES)

    low = lax.broadcasted_iota(jnp.int32, (1, LANES), 1) < LANES // 2

    def piece(d):
        return pl.ds(pl.multiple_of(d * share, 8), share)

    packed = share == padded
    size = upin.shape[0] // wide

    def note(i):
        return pl.ds(pl.multiple_of(i * size, 8), size)

    def write(ref, i, tile):
        if not packed:
            ref[note(i), :] = tile
            return
        third = (padded - PLAIN) // 3
        rest = tile[PLAIN:padded, :]
        most = jnp.maximum(jnp.max(jnp.abs(rest), 0, keepdims=True), F32(1e-30))
        fine = F32(FINE) / most
        one = jnp.floor(rest[0:third, :] * fine + F32(0.5))
        two = jnp.floor(rest[third : 2 * third, :] * (fine * F32(0.5)) + F32(0.5))
        three = jnp.floor(rest[2 * third :, :] * fine + F32(0.5))
        high = jnp.floor(two * F32(1.0 / 256.0))
        at = i * size
        ref[pl.ds(pl.multiple_of(at, 8), PLAIN), :] = tile[0:PLAIN, :]
        ref[pl.ds(at + PLAIN - 1, 1), :] = most
        ref[pl.ds(pl.multiple_of(at + PLAIN, 8), third), :] = one * F32(256.0) + (high + F32(128.0))
        ref[pl.ds(pl.multiple_of(at + PLAIN + third, 8), third), :] = three * F32(256.0) + (two - high * F32(256.0))

    def read(ref, i):
        if not packed:
            return ref[note(i), :]
        third = (padded - PLAIN) // 3
        at = i * size
        plain = ref[pl.ds(pl.multiple_of(at, 8), PLAIN), :]
        left = ref[pl.ds(pl.multiple_of(at + PLAIN, 8), third), :]
        right = ref[pl.ds(pl.multiple_of(at + PLAIN + third, 8), third), :]
        step = plain[PLAIN - 1 : PLAIN, :] * F32(1.0 / FINE)
        one = jnp.floor(left * F32(1.0 / 256.0))
        three = jnp.floor(right * F32(1.0 / 256.0))
        two = (left - one * F32(256.0) - F32(128.0)) * F32(256.0) + (right - three * F32(256.0))
        return jnp.concatenate([plain, one * step, two * (step * F32(2.0)), three * step], 0)

    def first(k):
        d = other(k)
        return pltpu.make_async_remote_copy(
            src_ref=state.at[piece(d), :], dst_ref=got.at[piece(mw), :],
            send_sem=send1.at[k], recv_sem=recv1.at[k],
            device_id={"wide": d, "narrow": mz}, device_id_type=MESH,
        )

    def second(i, sender):
        return pltpu.make_async_remote_copy(
            src_ref=scan.at[piece(i), :], dst_ref=prior.at[piece(mw), :],
            send_sem=send2.at[i], recv_sem=recv2.at[sender],
            device_id={"wide": i, "narrow": mz}, device_id_type=MESH,
        )

    def up(i):
        return pltpu.make_async_remote_copy(
            src_ref=upout.at[note(i), :], dst_ref=upin.at[note(i), :],
            send_sem=usend.at[i], recv_sem=urecv.at[i],
            device_id={"wide": mw, "narrow": lax.rem(mz + 1, narrow)}, device_id_type=MESH,
        )

    def down(i):
        return pltpu.make_async_remote_copy(
            src_ref=downout.at[note(i), :], dst_ref=downin.at[note(i), :],
            send_sem=dsend.at[i], recv_sem=drecv.at[i],
            device_id={"wide": mw, "narrow": lax.rem(mz + narrow - 1, narrow)}, device_id_type=MESH,
        )

    def rim(p, which):
        src, dst = ((wk_in, rimk), (val_in, rimv))[which]
        return pltpu.make_async_remote_copy(
            src_ref=src.at[:, cols(p)], dst_ref=dst.at[p],
            send_sem=rsend.at[which, p], recv_sem=rrecv.at[which, p],
            device_id=where_is(lax.rem(me + 1, n)), device_id_type=MESH,
        )

    def rims(lo, hi):
        @pl.when(not_last)
        def _():
            @pl.loop(lo, hi)
            def _(p):
                rim(p, 0).start()
                rim(p, 1).start()

    def early(z):
        return jnp.minimum(jnp.where(z == narrow - 1, 0, EARLY + MORE * z), pairs)

    far = jnp.where(lax.rem(mw, 2) == 0, FAR, 0)

    def keys(p):
        x = fk[:, cols(lax.div(2 * p, per))]
        v = val[:, cols(p)]
        base = pl.multiple_of(p * padded, 8)
        parts = []
        norms = []
        for e in range(2):
            j = lax.rem(2 * p + e, per)
            a = nt(pick[0, j], x) + ccol[:, 0:1]
            b = nt(pick[1, j], x) + ccol[:, 1:2]
            k = (a * b * ccol[:, 2:3]).astype(BF16)
            kft[2 * p + e] = k
            parts.append(nn(k, v))
            norms.append(nt(jnp.ones((8, rows), BF16), k))
        state[pl.ds(base, padded), :] = jnp.where(low, parts[0], parts[1])
        for e in range(2):
            state[pl.ds(base + NORMS + 2 * e, 1), :] = norms[e][0:1, 0:LANES]
            state[pl.ds(base + NORMS + 2 * e + 1, 1), 0 : padded - LANES] = norms[e][0:1, LANES:padded]

    def batch(g):
        return [lax.rem(lax.div(mw, chop) + 1 + g * GROUP + j, pairs) for j in range(GROUP)]

    def share_out(g):
        for p in batch(g):
            for e in range(chop):
                d = p * chop + e

                @pl.when(d != mw)
                def _():
                    first(lax.rem(d - mw + wide, wide)).start()

    for one in loads[:4]:
        one.wait()
    for p in batch(0):
        keys(p)
    pl.semaphore_wait(barrier, wide - 1 + (mz > 0) + jnp.logical_not(top_z) + (top_z & not_last) + ((mz == 0) & (me > 0)))
    share_out(0)
    rims(0, early(mz))

    @pl.when(top_z)
    def _():
        rims(0, far)

    @pl.loop(1, pairs // GROUP)
    def _(g):
        for p in batch(g):
            keys(p)
        share_out(g)

    got[piece(mw), :] = state[piece(mw), :]
    for one in loads[4:]:
        one.wait()

    r = lax.broadcasted_iota(jnp.int32, (rows, rows), 0)
    c = lax.broadcasted_iota(jnp.int32, (rows, rows), 1)
    causal = r >= c

    def intra(p):
        x = fq[:, cols(lax.div(2 * p, per))]
        v = val[:, cols(p)]
        nums = []
        dens = []
        for e in range(2):
            j = lax.rem(2 * p + e, per)
            a = nt(x, pick[0, j]) + crow[0:1, :]
            b = nt(x, pick[1, j]) + crow[1:2, :]
            q = (a * b * crow[2:3, :]).astype(BF16)
            qf[2 * p + e] = q
            s = jnp.where(causal, nn(q, kft[2 * p + e]), F32(0.0))
            dens.append(jnp.sum(s, -1, keepdims=True))
            nums.append(nn(s.astype(BF16), v))
        num[:, cols(p)] = jnp.where(low, nums[0], nums[1])
        den[:, cols(p)] = jnp.where(low, dens[0], dens[1])

    @pl.loop(0, AHEAD, unroll=2)
    def _(p):
        intra(p)

    @pl.loop(1, wide)
    def _(k):
        first(k).wait_recv()

    def add(d, total):
        scan[piece(d), :] = total
        total = total + got[piece(d), :]
        got[piece(d), :] = total
        return total

    lax.fori_loop(0, wide, add, jnp.zeros((share, LANES), F32))

    scale = BF16(1.0 / np.sqrt(LANES // 2))
    rim_ok = (c > r) & (me > 0)

    def attend(p):
        @pl.when(me > 0)
        def _():
            rim(p, 0).wait_recv()
            rim(p, 1).wait_recv()

        q = wq[:, cols(p)] * scale
        k = wk[:, cols(p)]
        v = val[:, cols(p)]
        rk = rimk[p]
        rv = rimv[p]
        outs = []
        for e in range(2):
            qe = jnp.where(low if e == 0 else ~low, q, jnp.zeros_like(q))
            s0 = jnp.where(rim_ok, nt(qe, rk), F32(-1e30))
            s1 = jnp.where(causal, nt(qe, k), F32(-1e30))
            m = jnp.maximum(jnp.max(s0, -1, keepdims=True), jnp.max(s1, -1, keepdims=True))
            e0 = jnp.exp(s0 - m)
            e1 = jnp.exp(s1 - m)
            inv = F32(1.0) / (jnp.sum(e0, -1, keepdims=True) + jnp.sum(e1, -1, keepdims=True))
            outs.append(nn((e0 * inv).astype(BF16), rv) + nn((e1 * inv).astype(BF16), v))
        return jnp.where(low, outs[0], outs[1])

    lead = LAG * jnp.maximum(mz, narrow - 1 - mz)
    spent = wide - 1 + LAG * mz

    @pl.when(mz == 0)
    def _():
        @pl.loop(0, wide)
        def _(i):
            write(upout, i, got[piece(i), :])
            up(i).start()

        rims(early(mz), pairs)

    @pl.when(top_z)
    def _():
        @pl.loop(1, wide)
        def _(j):
            write(downout, j, scan[piece(j), :])
            down(j).start()

    def slot(t):
        i = t - LAG * mz

        @pl.when((i >= 0) & (i < wide) & (mz > 0))
        def _():
            up(i).wait_recv()

            @pl.when(mz < narrow - 1)
            def _():
                write(upout, i, read(upin, i) + got[piece(i), :])
                up(i).start()

        j = t - LAG * (narrow - 1 - mz)

        @pl.when((j >= 1) & (j < wide) & (mz < narrow - 1))
        def _():
            down(j).wait_recv()

            @pl.when(mz > 0)
            def _():
                write(downout, j, read(downin, j) + scan[piece(j), :])
                down(j).start()

        o = t - lead

        @pl.when((o >= 0) & (o < wide))
        def _():
            scan[piece(o), :] = scan[piece(o), :] + read(upin, o) + read(downin, o)

            @pl.when(o == mw)
            def _():
                prior[piece(o), :] = scan[piece(o), :]

            @pl.when(o != mw)
            def _():
                second(o, mw).start()

        @pl.when((t == spent) & (mz > 0) & (mz < narrow - 1))
        def _():
            rims(early(mz), pairs)

        @pl.when(top_z & (t == PACE))
        def _():
            rims(far, pairs)

    slots = wide + LAG * (narrow - 1)
    rest = pairs - AHEAD
    due = jnp.where(mz > 0, early(mz - 1), jnp.where(lax.rem(mw, 2) == 1, FAR, 0))
    done = jnp.minimum(due, slots - rest)

    @pl.loop(0, slots)
    def _(t):
        slot(t)

        @pl.when(t < rest)
        def _():
            intra(AHEAD + t)

        @pl.when((t >= rest) & (t - rest < done))
        def _():
            held[:, cols(t - rest)] = attend(t - rest)

    @pl.loop(1, wide)
    def _(k):
        second(other(k), other(k)).wait_recv()

    @pl.loop(0, pairs, unroll=4)
    def _(p):
        base = pl.multiple_of(p * padded, 8)
        tile = prior[pl.ds(base, padded), :]
        hi = tile.astype(BF16)
        mid = (tile - hi.astype(F32)).astype(BF16)
        crosses = []
        dens = []
        for e in range(2):
            qe = qf[2 * p + e]
            crosses.append(nn(qe, hi) + nn(qe, mid))
            at = NORMS + 2 * e
            z0 = tile[at : at + 1, :]
            z1 = tile[at + 1 : at + 2, 0 : padded - LANES]
            q32 = qe.astype(F32)
            dens.append(
                jnp.sum(q32[:, 0:LANES] * z0, -1, keepdims=True)
                + jnp.sum(q32[:, LANES:padded] * z1, -1, keepdims=True)
            )
        top = num[:, cols(p)] + jnp.where(low, crosses[0], crosses[1])
        bottom = den[:, cols(p)] + jnp.where(low, dens[0], dens[1])
        num[:, cols(p)] = top / bottom

    @pl.loop(0, done)
    def _(p):
        out[:, cols(p)] = (num[:, cols(p)] + held[:, cols(p)]).astype(out.dtype)

    @pl.loop(done, pairs)
    def _(p):
        out[:, cols(p)] = (num[:, cols(p)] + attend(p)).astype(out.dtype)

    @pl.loop(1, wide)
    def _(k):
        first(k).wait_send()
        second(other(k), mw).wait_send()

    @pl.loop(0, wide)
    def _(i):
        @pl.when(mz < narrow - 1)
        def _():
            up(i).wait_send()

        @pl.when((mz > 0) & (i > 0))
        def _():
            down(i).wait_send()

    @pl.when(not_last)
    def _():
        @pl.loop(0, pairs)
        def _(p):
            rim(p, 0).wait_send()
            rim(p, 1).wait_send()


def solution(mesh):
    wide, narrow = mesh.shape["wide"], mesh.shape["narrow"]

    def body(feat_queries, feat_keys, values, window_queries, window_keys):
        rows, channels = values.shape
        assert rows == WINDOW and channels == HEADS * LANES // 2
        padded, per, pick, extra = tables(feat_queries.shape[1] // HEADS)
        pairs = channels // LANES
        share = -(-pairs * padded // (8 * wide)) * 8
        whole = pltpu.VMEM((wide * share, LANES), F32)
        plain = layout(feat_queries.shape[1] // HEADS)[1]
        size = plain + (padded - plain) // 3 * 2 if share == padded else share
        notes = pltpu.VMEM((wide * size, LANES), F32)
        assert padded % share == 0
        vmem = pl.BlockSpec(memory_space=pltpu.VMEM)
        ins = (
            feat_queries, feat_keys, values, window_queries, window_keys,
            jnp.asarray(pick, BF16), jnp.asarray(extra, F32), jnp.asarray(extra.T, F32),
        )
        return pl.pallas_call(
            functools.partial(kernel, (wide, narrow, padded, per, share)),
            out_shape=jax.ShapeDtypeStruct((rows, channels), BF16),
            in_specs=[pl.BlockSpec(memory_space=pltpu.HBM)] * 8,
            out_specs=vmem,
            scratch_shapes=[
                *[pltpu.VMEM(one.shape, one.dtype) for one in ins],
                pltpu.VMEM((HEADS, rows, padded), BF16),
                pltpu.VMEM((HEADS, padded, rows), BF16),
                *[whole] * 2,
                *[notes] * 4,
                *[whole] * 2,
                pltpu.VMEM((pairs, rows, LANES), BF16),
                pltpu.VMEM((pairs, rows, LANES), BF16),
                pltpu.VMEM((rows, channels), F32),
                pltpu.VMEM((rows, channels), F32),
                pltpu.VMEM((rows, channels), F32),
                pltpu.SemaphoreType.DMA((8,)),
                *[pltpu.SemaphoreType.DMA((wide,))] * 8,
                pltpu.SemaphoreType.DMA((2, pairs)),
                pltpu.SemaphoreType.DMA((2, pairs)),
            ],
            compiler_params=pltpu.CompilerParams(
                collective_id=0, has_side_effects=True, vmem_limit_bytes=56 * 1024 * 1024
            ),
        )(*ins)

    spec = P(("wide", "narrow"), None)
    return jax.shard_map(
        body, mesh=mesh, in_specs=(spec,) * 5, out_specs=spec, check_vma=False
    )
```

```python
import functools

import jax
import jax.numpy as jnp
import numpy as np
from jax import lax
from jax.experimental import pallas as pl
from jax.experimental.pallas import tpu as pltpu
from jax.sharding import PartitionSpec as P

HEADS = 16
WINDOW = 256
LANES = 128
EARLY = 2
MORE = 1
AHEAD = 4
GROUP = 2
FAR = 5
PACE = 10
MIX = 0
STEP = 1
BURST = 1
RATE = 1
LAG = 2
FINE = 65000.0
MESH = pl.DeviceIdType.MESH
F32 = jnp.float32
BF16 = jnp.bfloat16
NT = (((1,), (1,)), ((), ()))


def nt(a, b):
    return lax.dot_general(a, b, NT, preferred_element_type=F32)


def nn(a, b):
    return jnp.dot(a, b, preferred_element_type=F32)


def layout(width):
    norms = 1 + 2 * width
    return norms, -(-(norms + 5) // 8) * 8


def tables(width):
    norms, plain = layout(width)
    pairs = [(i, i) for i in range(width)] + [(i, j) for i in range(width) for j in range(i + 1, width)]
    padded = plain + -(-(len(pairs) - width) // 24) * 24
    per = LANES // width
    one = np.zeros((padded, width))
    two = np.zeros((padded, width))
    extra = np.zeros((8, padded))
    extra[0, 0] = 1.0
    extra[1, : 1 + width] = 1.0
    extra[2, 0] = 1.0
    extra[2, 1 : 1 + width] = 1.0 / width**0.25
    for i in range(width):
        one[1 + i, i] = 1.0
    for n, (i, j) in enumerate(pairs):
        at = 1 + width + n if n < width else plain + n - width
        one[at, i] = 1.0
        two[at, j] = 1.0
        extra[2, at] = 1.0 / np.sqrt(2.0 * width) if i == j else 1.0 / np.sqrt(1.0 * width)
    pick = np.zeros((2, per, padded, LANES))
    for j in range(per):
        pick[0, j, :, j * width : (j + 1) * width] = one
        pick[1, j, :, j * width : (j + 1) * width] = two
    return padded, per, pick, extra


def kernel(
    dims,
    fq_in, fk_in, val_in, wq_in, wk_in, pick_in, crow_in, ccol_in,
    out,
    fq, fk, val, wq, wk, pick, crow, ccol,
    qf, kft, own, scan, state, got, upin, upout, downin, downout, base, prior,
    rimk, rimv, farsk, farsv, num, den, held,
    load, send1, recv1, send2, recv2, usend, urecv, dsend, drecv, rsend, rrecv, hrecv, psend,
):
    wide, narrow, padded, per, share = dims
    NORMS, PLAIN = layout(fq_in.shape[1] // HEADS)
    n = wide * narrow
    rows = val.shape[0]
    pairs = val.shape[1] // LANES
    chop = padded // share
    mw = lax.axis_index("wide")
    mz = lax.axis_index("narrow")
    me = mw * narrow + mz
    top_z = mz == narrow - 1
    not_last = me < n - 1

    ins = (fk_in, pick_in, ccol_in, val_in, fq_in, crow_in, wq_in, wk_in)
    mine = (fk, pick, ccol, val, fq, crow, wq, wk)
    loads = [pltpu.make_async_copy(i, m, load.at[j]) for j, (i, m) in enumerate(zip(ins, mine))]
    for one in loads:
        one.start()

    def where_is(d):
        return {"wide": lax.div(d, narrow), "narrow": lax.rem(d, narrow)}

    def other(k):
        return lax.rem(mw + k, wide)

    barrier = pltpu.get_barrier_semaphore()

    def greet(d):
        pl.semaphore_signal(barrier, inc=1, device_id=d, device_id_type=MESH)

    @pl.loop(1, wide)
    def _(k):
        greet({"wide": other(k), "narrow": mz})

    @pl.when(jnp.logical_not(top_z))
    def _():
        greet({"wide": mw, "narrow": mz + 1})

    @pl.when(mz > 0)
    def _():
        greet({"wide": mw, "narrow": mz - 1})

    even = lax.rem(mw, 2) == 0
    ahead_of = top_z & even & (mw < wide - 1)
    passes = top_z & even & (mw > 0)
    hands = top_z & jnp.logical_not(even) & (mw < wide - 1)
    plain_rim = not_last & jnp.logical_not(hands)

    @pl.when(ahead_of)
    def _():
        greet({"wide": mw + 1, "narrow": 0})

    @pl.when(passes)
    def _():
        greet({"wide": mw, "narrow": 0})

    @pl.when((mz == 0) & (mw > 0))
    def _():
        greet({"wide": jnp.where(even, mw, mw - 1), "narrow": narrow - 1})

    @pl.when(mz == 0)
    def _():
        upin[...] = jnp.zeros_like(upin)

    @pl.when(top_z)
    def _():
        downin[...] = jnp.zeros_like(downin)

    downin[pl.ds(0, upin.shape[0] // wide), :] = jnp.zeros((upin.shape[0] // wide, LANES), F32)

    @pl.when(me == 0)
    def _():
        rimk[...] = jnp.zeros_like(rimk)
        rimv[...] = jnp.zeros_like(rimv)

    def cols(p):
        return pl.ds(pl.multiple_of(p * LANES, LANES), LANES)

    low = lax.broadcasted_iota(jnp.int32, (1, LANES), 1) < LANES // 2

    def piece(d):
        return pl.ds(pl.multiple_of(d * share, 8), share)

    packed = share == padded
    size = upin.shape[0] // wide

    def note(i):
        return pl.ds(pl.multiple_of(i * size, 8), size)

    def write(ref, i, tile):
        if not packed:
            ref[note(i), :] = tile
            return
        third = (padded - PLAIN) // 3
        rest = tile[PLAIN:padded, :]
        most = jnp.maximum(jnp.max(jnp.abs(rest), 0, keepdims=True), F32(1e-30))
        fine = F32(FINE) / most
        one = jnp.floor(rest[0:third, :] * fine + F32(0.5))
        two = jnp.floor(rest[third : 2 * third, :] * (fine * F32(0.5)) + F32(0.5))
        three = jnp.floor(rest[2 * third :, :] * fine + F32(0.5))
        high = jnp.floor(two * F32(1.0 / 256.0))
        at = i * size
        ref[pl.ds(pl.multiple_of(at, 8), PLAIN), :] = tile[0:PLAIN, :]
        ref[pl.ds(at + PLAIN - 1, 1), :] = most
        ref[pl.ds(pl.multiple_of(at + PLAIN, 8), third), :] = one * F32(256.0) + (high + F32(128.0))
        ref[pl.ds(pl.multiple_of(at + PLAIN + third, 8), third), :] = three * F32(256.0) + (two - high * F32(256.0))

    def read(ref, i):
        if not packed:
            return ref[note(i), :]
        third = (padded - PLAIN) // 3
        at = i * size
        plain = ref[pl.ds(pl.multiple_of(at, 8), PLAIN), :]
        left = ref[pl.ds(pl.multiple_of(at + PLAIN, 8), third), :]
        right = ref[pl.ds(pl.multiple_of(at + PLAIN + third, 8), third), :]
        step = plain[PLAIN - 1 : PLAIN, :] * F32(1.0 / FINE)
        one = jnp.floor(left * F32(1.0 / 256.0))
        three = jnp.floor(right * F32(1.0 / 256.0))
        two = (left - one * F32(256.0) - F32(128.0)) * F32(256.0) + (right - three * F32(256.0))
        return jnp.concatenate([plain, one * step, two * (step * F32(2.0)), three * step], 0)

    def first(k):
        d = other(k)
        return pltpu.make_async_remote_copy(
            src_ref=state.at[note(d), :], dst_ref=got.at[note(mw), :],
            send_sem=send1.at[k], recv_sem=recv1.at[k],
            device_id={"wide": d, "narrow": mz}, device_id_type=MESH,
        )

    def second(i, sender):
        return pltpu.make_async_remote_copy(
            src_ref=base.at[note(i), :], dst_ref=prior.at[note(mw), :],
            send_sem=send2.at[i], recv_sem=recv2.at[sender],
            device_id={"wide": i, "narrow": mz}, device_id_type=MESH,
        )

    def up(i):
        return pltpu.make_async_remote_copy(
            src_ref=upout.at[note(i), :], dst_ref=upin.at[note(i), :],
            send_sem=usend.at[i], recv_sem=urecv.at[i],
            device_id={"wide": mw, "narrow": lax.rem(mz + 1, narrow)}, device_id_type=MESH,
        )

    def down(i):
        return pltpu.make_async_remote_copy(
            src_ref=downout.at[note(i), :], dst_ref=downin.at[note(i), :],
            send_sem=dsend.at[i], recv_sem=drecv.at[i],
            device_id={"wide": mw, "narrow": lax.rem(mz + narrow - 1, narrow)}, device_id_type=MESH,
        )

    def rim(p, which):
        src, dst = ((wk_in, rimk), (val_in, rimv))[which]
        return pltpu.make_async_remote_copy(
            src_ref=src.at[:, cols(p)], dst_ref=dst.at[p],
            send_sem=rsend.at[which, p], recv_sem=rrecv.at[which, p],
            device_id=where_is(lax.rem(me + 1, n)), device_id_type=MESH,
        )

    def hand(p, which):
        src, dst = ((wk_in, farsk), (val_in, farsv))[which]
        return pltpu.make_async_remote_copy(
            src_ref=src.at[:, cols(p)], dst_ref=dst.at[p],
            send_sem=rsend.at[which, p], recv_sem=hrecv.at[which, p],
            device_id={"wide": other(1), "narrow": mz}, device_id_type=MESH,
        )

    def relay(p, which):
        src, dst = ((farsk, rimk), (farsv, rimv))[which]
        return pltpu.make_async_remote_copy(
            src_ref=src.at[p], dst_ref=dst.at[p],
            send_sem=psend.at[which, p], recv_sem=rrecv.at[which, p],
            device_id={"wide": mw, "narrow": 0}, device_id_type=MESH,
        )

    def rims(lo, hi):
        @pl.when(plain_rim)
        def _():
            @pl.loop(lo, hi)
            def _(p):
                rim(p, 0).start()
                rim(p, 1).start()

    def early(z):
        return jnp.minimum(jnp.where(z == narrow - 1, 0, EARLY + MORE * z), pairs)

    far = jnp.where(lax.rem(mw, 2) == 0, FAR, 0)

    def keys(p):
        x = fk[:, cols(lax.div(2 * p, per))]
        v = val[:, cols(p)]
        at = pl.multiple_of(p * padded, 8)
        parts = []
        norms = []
        for e in range(2):
            j = lax.rem(2 * p + e, per)
            a = nt(pick[0, j], x) + ccol[:, 0:1]
            b = nt(pick[1, j], x) + ccol[:, 1:2]
            k = (a * b * ccol[:, 2:3]).astype(BF16)
            kft[2 * p + e] = k
            parts.append(nn(k, v))
            norms.append(nt(jnp.ones((8, rows), BF16), k))
        own[pl.ds(at, padded), :] = jnp.where(low, parts[0], parts[1])
        for e in range(2):
            own[pl.ds(at + NORMS + 2 * e, 1), :] = norms[e][0:1, 0:LANES]
            own[pl.ds(at + NORMS + 2 * e + 1, 1), 0 : padded - LANES] = norms[e][0:1, LANES:padded]
        for e in range(chop):
            write(state, p * chop + e, own[piece(p * chop + e), :])

    def batch(g):
        return [lax.rem(lax.div(mw, chop) + 1 + g * GROUP + j, pairs) for j in range(GROUP)]

    def share_out(g):
        for p in batch(g):
            for e in range(chop):
                d = p * chop + e

                @pl.when(d != mw)
                def _():
                    first(lax.rem(d - mw + wide, wide)).start()

    for one in loads[:4]:
        one.wait()
    for p in batch(0):
        keys(p)
    pl.semaphore_wait(barrier, wide - 1 + (mz > 0) + jnp.logical_not(top_z) + ahead_of + passes + ((mz == 0) & (mw > 0)))
    share_out(0)
    rims(0, early(mz))

    @pl.when(top_z)
    def _():
        rims(0, far)

    @pl.loop(1, pairs // GROUP)
    def _(g):
        for p in batch(g):
            keys(p)
        share_out(g)

    for one in loads[4:]:
        one.wait()

    r = lax.broadcasted_iota(jnp.int32, (rows, rows), 0)
    c = lax.broadcasted_iota(jnp.int32, (rows, rows), 1)
    causal = r >= c

    def intra(p):
        x = fq[:, cols(lax.div(2 * p, per))]
        v = val[:, cols(p)]
        nums = []
        dens = []
        for e in range(2):
            j = lax.rem(2 * p + e, per)
            a = nt(x, pick[0, j]) + crow[0:1, :]
            b = nt(x, pick[1, j]) + crow[1:2, :]
            q = (a * b * crow[2:3, :]).astype(BF16)
            qf[2 * p + e] = q
            s = jnp.where(causal, nn(q, kft[2 * p + e]), F32(0.0))
            dens.append(jnp.sum(s, -1, keepdims=True))
            nums.append(nn(s.astype(BF16), v))
        num[:, cols(p)] = jnp.where(low, nums[0], nums[1])
        den[:, cols(p)] = jnp.where(low, dens[0], dens[1])

    @pl.loop(0, AHEAD, unroll=2)
    def _(p):
        intra(p)

    @pl.loop(1, wide)
    def _(k):
        first(k).wait_recv()

    mine_tile = own[piece(mw), :]

    def add(d, total):
        scan[piece(d), :] = total
        total = total + jnp.where(d == mw, mine_tile, read(got, d))
        own[piece(d), :] = total
        return total

    lax.fori_loop(0, wide, add, jnp.zeros((share, LANES), F32))

    scale = BF16(1.0 / np.sqrt(LANES // 2))
    rim_ok = (c > r) & (me > 0)

    def attend(p):
        @pl.when(me > 0)
        def _():
            rim(p, 0).wait_recv()
            rim(p, 1).wait_recv()

        q = wq[:, cols(p)] * scale
        k = wk[:, cols(p)]
        v = val[:, cols(p)]
        rk = rimk[p]
        rv = rimv[p]
        outs = []
        for e in range(2):
            qe = jnp.where(low if e == 0 else ~low, q, jnp.zeros_like(q))
            s0 = jnp.where(rim_ok, nt(qe, rk), F32(-1e30))
            s1 = jnp.where(causal, nt(qe, k), F32(-1e30))
            m = jnp.maximum(jnp.max(s0, -1, keepdims=True), jnp.max(s1, -1, keepdims=True))
            e0 = jnp.exp(s0 - m)
            e1 = jnp.exp(s1 - m)
            inv = F32(1.0) / (jnp.sum(e0, -1, keepdims=True) + jnp.sum(e1, -1, keepdims=True))
            outs.append(nn((e0 * inv).astype(BF16), rv) + nn((e1 * inv).astype(BF16), v))
        return jnp.where(low, outs[0], outs[1])

    lead = LAG * jnp.maximum(mz, narrow - 1 - mz)
    spent = wide - 1 + LAG * mz

    @pl.when(mz == 0)
    def _():
        @pl.loop(0, wide)
        def _(i):
            write(upout, i, own[piece(i), :])
            up(i).start()

        rims(early(mz), pairs)

    @pl.when(hands)
    def _():
        @pl.loop(0, pairs)
        def _(p):
            hand(p, 0).start()
            hand(p, 1).start()


    left = 2 * (pairs - FAR)
    mixed = (wide - 1 - MIX) * BURST

    def either(make, q, act):
        for which in range(2):

            @pl.when(lax.rem(q, 2) == which)
            def _():
                act(make(lax.div(q, 2), which))

    def flow(q):
        @pl.when(ahead_of & (q < left))
        def _():
            either(rim, 2 * FAR + q, lambda copy: copy.start())

        @pl.when(passes & (q >= left) & (q < left + 2 * pairs))
        def _():
            either(hand, q - left, lambda copy: copy.wait_recv())
            either(relay, q - left, lambda copy: copy.start())

    def slot(t):
        @pl.when(top_z & (t < wide - 1))
        def _():
            write(downout, t + 1, scan[piece(t + 1), :])
            down(t + 1).start()

            @pl.when(even & (t >= MIX))
            def _():
                for e in range(BURST):
                    flow((t - MIX) * BURST + e)

        @pl.when(top_z & even & (t >= PACE) & (lax.rem(t - PACE, STEP) == 0))
        def _():
            for e in range(RATE):
                flow(mixed + lax.div(t - PACE, STEP) * RATE + e)

        i = t - LAG * mz

        @pl.when((i >= 0) & (i < wide) & (mz > 0))
        def _():
            up(i).wait_recv()

            @pl.when(mz < narrow - 1)
            def _():
                write(upout, i, read(upin, i) + own[piece(i), :])
                up(i).start()

        j = t - LAG * (narrow - 1 - mz)

        @pl.when((j >= 1) & (j < wide) & (mz < narrow - 1))
        def _():
            down(j).wait_recv()

            @pl.when(mz > 0)
            def _():
                write(downout, j, read(downin, j) + scan[piece(j), :])
                down(j).start()

        o = t - lead

        @pl.when((o >= 0) & (o < wide))
        def _():
            tile = scan[piece(o), :] + read(upin, o) + read(downin, o)

            @pl.when(o == mw)
            def _():
                write(prior, o, tile)

            @pl.when(o != mw)
            def _():
                write(base, o, tile)
                second(o, mw).start()

        @pl.when((t == spent) & (mz > 0) & (mz < narrow - 1))
        def _():
            rims(early(mz), pairs)

    slots = wide + LAG * (narrow - 1)
    rest = pairs - AHEAD
    due = jnp.where(mz > 0, early(mz - 1), jnp.where(lax.rem(mw, 2) == 1, FAR, 0))
    done = jnp.minimum(due, slots - rest)

    @pl.loop(0, slots)
    def _(t):
        slot(t)

        @pl.when(t < rest)
        def _():
            intra(AHEAD + t)

        @pl.when((t >= rest) & (t - rest < done))
        def _():
            held[:, cols(t - rest)] = attend(t - rest)

    @pl.when(top_z & even)
    def _():
        @pl.loop(mixed + max(0, -(-(slots - PACE) // STEP)) * RATE, left + 2 * pairs)
        def _(q):
            flow(q)

    @pl.loop(1, wide)
    def _(k):
        second(other(k), other(k)).wait_recv()

    @pl.loop(0, pairs, unroll=4)
    def _(p):
        tile = jnp.concatenate([read(prior, p * chop + e) for e in range(chop)], 0)
        hi = tile.astype(BF16)
        mid = (tile - hi.astype(F32)).astype(BF16)
        crosses = []
        dens = []
        for e in range(2):
            qe = qf[2 * p + e]
            crosses.append(nn(qe, hi) + nn(qe, mid))
            at = NORMS + 2 * e
            z0 = tile[at : at + 1, :]
            z1 = tile[at + 1 : at + 2, 0 : padded - LANES]
            q32 = qe.astype(F32)
            dens.append(
                jnp.sum(q32[:, 0:LANES] * z0, -1, keepdims=True)
                + jnp.sum(q32[:, LANES:padded] * z1, -1, keepdims=True)
            )
        top = num[:, cols(p)] + jnp.where(low, crosses[0], crosses[1])
        bottom = den[:, cols(p)] + jnp.where(low, dens[0], dens[1])
        num[:, cols(p)] = top / bottom

    @pl.loop(0, done)
    def _(p):
        out[:, cols(p)] = (num[:, cols(p)] + held[:, cols(p)]).astype(out.dtype)

    @pl.loop(1, wide)
    def _(k):
        first(k).wait_send()
        second(other(k), mw).wait_send()

    @pl.loop(0, wide)
    def _(i):
        @pl.when(mz < narrow - 1)
        def _():
            up(i).wait_send()

        @pl.when((mz > 0) & (i > 0))
        def _():
            down(i).wait_send()

    @pl.loop(done, pairs)
    def _(p):
        out[:, cols(p)] = (num[:, cols(p)] + attend(p)).astype(out.dtype)

    @pl.when(not_last)
    def _():
        @pl.loop(0, pairs)
        def _(p):
            rim(p, 0).wait_send()
            rim(p, 1).wait_send()

    @pl.when(passes)
    def _():
        @pl.loop(0, pairs)
        def _(p):
            relay(p, 0).wait_send()
            relay(p, 1).wait_send()


def solution(mesh):
    wide, narrow = mesh.shape["wide"], mesh.shape["narrow"]

    def body(feat_queries, feat_keys, values, window_queries, window_keys):
        rows, channels = values.shape
        assert rows == WINDOW and channels == HEADS * LANES // 2
        padded, per, pick, extra = tables(feat_queries.shape[1] // HEADS)
        pairs = channels // LANES
        share = -(-pairs * padded // (8 * wide)) * 8
        whole = pltpu.VMEM((wide * share, LANES), F32)
        plain = layout(feat_queries.shape[1] // HEADS)[1]
        size = plain + (padded - plain) // 3 * 2 if share == padded else share
        notes = pltpu.VMEM((wide * size, LANES), F32)
        assert padded % share == 0
        ins = (
            feat_queries, feat_keys, values, window_queries, window_keys,
            jnp.asarray(pick, BF16), jnp.asarray(extra, F32), jnp.asarray(extra.T, F32),
        )
        ins = tuple(pltpu.with_memory_space_constraint(one, pltpu.HBM) for one in ins)
        return pl.pallas_call(
            functools.partial(kernel, (wide, narrow, padded, per, share)),
            out_shape=jax.ShapeDtypeStruct((rows, channels), BF16),
            in_specs=[pl.BlockSpec(memory_space=pltpu.HBM)] * 8,
            out_specs=pl.BlockSpec(memory_space=pltpu.VMEM),
            scratch_shapes=[
                *[pltpu.VMEM(one.shape, one.dtype) for one in ins],
                pltpu.VMEM((HEADS, rows, padded), BF16),
                pltpu.VMEM((HEADS, padded, rows), BF16),
                *[whole] * 2,
                *[notes] * 8,
                *[pltpu.VMEM((pairs, rows, LANES), BF16)] * 4,
                *[pltpu.VMEM((rows, channels), F32)] * 3,
                pltpu.SemaphoreType.DMA((8,)),
                *[pltpu.SemaphoreType.DMA((wide,))] * 8,
                *[pltpu.SemaphoreType.DMA((2, pairs))] * 4,
            ],
            compiler_params=pltpu.CompilerParams(
                collective_id=0, has_side_effects=True, vmem_limit_bytes=40 * 1024 * 1024
            ),
        )(*ins)

    spec = P(("wide", "narrow"), None)
    return jax.shard_map(
        body, mesh=mesh, in_specs=(spec,) * 5, out_specs=spec, check_vma=False
    )
```

```python
import functools

import jax
import jax.numpy as jnp
import numpy as np
from jax import lax
from jax.experimental import pallas as pl
from jax.experimental.pallas import tpu as pltpu
from jax.sharding import PartitionSpec as P

HEADS = 16
WINDOW = 256
LANES = 128
EARLY = 2
MORE = 1
AHEAD = 4
GROUP = 2
FAR = 5
PACE = 9
MIX = 0
STEP = 1
BURST = 1
RATE = 1
LAG = 2
FIRST = 2
DIRECT = 5
KEEP = 0
FINE = 65000.0
MESH = pl.DeviceIdType.MESH
F32 = jnp.float32
BF16 = jnp.bfloat16
NT = (((1,), (1,)), ((), ()))


def nt(a, b):
    return lax.dot_general(a, b, NT, preferred_element_type=F32)


def nn(a, b):
    return jnp.dot(a, b, preferred_element_type=F32)


def layout(width):
    norms = 1 + 2 * width
    return norms, -(-(norms + 5) // 8) * 8


def tables(width):
    norms, plain = layout(width)
    pairs = [(i, i) for i in range(width)] + [(i, j) for i in range(width) for j in range(i + 1, width)]
    padded = plain + -(-(len(pairs) - width) // 24) * 24
    per = LANES // width
    one = np.zeros((padded, width))
    two = np.zeros((padded, width))
    extra = np.zeros((8, padded))
    extra[0, 0] = 1.0
    extra[1, : 1 + width] = 1.0
    extra[2, 0] = 1.0
    extra[2, 1 : 1 + width] = 1.0 / width**0.25
    for i in range(width):
        one[1 + i, i] = 1.0
    for n, (i, j) in enumerate(pairs):
        at = 1 + width + n if n < width else plain + n - width
        one[at, i] = 1.0
        two[at, j] = 1.0
        extra[2, at] = 1.0 / np.sqrt(2.0 * width) if i == j else 1.0 / np.sqrt(1.0 * width)
    pick = np.zeros((2, per, padded, LANES))
    for j in range(per):
        pick[0, j, :, j * width : (j + 1) * width] = one
        pick[1, j, :, j * width : (j + 1) * width] = two
    return padded, per, pick, extra


def kernel(
    dims,
    fq_in, fk_in, val_in, wq_in, wk_in, pick_in, crow_in, ccol_in,
    out,
    fq, fk, val, wq, wk, pick, crow, ccol,
    qf, kft, own, scan, state, got, upin, upout, downin, downout, base, prior,
    rimk, rimv, farsk, farsv, num, den, held, expo, peak, mass,
    load, send1, recv1, send2, recv2, usend, urecv, dsend, drecv, rsend, rrecv, hrecv, psend,
):
    wide, narrow, padded, per, share = dims
    NORMS, PLAIN = layout(fq_in.shape[1] // HEADS)
    n = wide * narrow
    rows = val.shape[0]
    pairs = val.shape[1] // LANES
    chop = padded // share
    mw = lax.axis_index("wide")
    mz = lax.axis_index("narrow")
    me = mw * narrow + mz
    top_z = mz == narrow - 1
    not_last = me < n - 1

    ins = (fk_in, pick_in, ccol_in, val_in, fq_in, crow_in, wq_in, wk_in)
    mine = (fk, pick, ccol, val, fq, crow, wq, wk)
    loads = [pltpu.make_async_copy(i, m, load.at[j]) for j, (i, m) in enumerate(zip(ins, mine))]
    for one in loads:
        one.start()

    def where_is(d):
        return {"wide": lax.div(d, narrow), "narrow": lax.rem(d, narrow)}

    def other(k):
        return lax.rem(mw + k, wide)

    barrier = pltpu.get_barrier_semaphore()

    def greet(d):
        pl.semaphore_signal(barrier, inc=1, device_id=d, device_id_type=MESH)

    @pl.loop(1, wide)
    def _(k):
        greet({"wide": other(k), "narrow": mz})

    @pl.when(jnp.logical_not(top_z))
    def _():
        greet({"wide": mw, "narrow": mz + 1})

    @pl.when(mz > 0)
    def _():
        greet({"wide": mw, "narrow": mz - 1})

    even = lax.rem(mw, 2) == 0
    ahead_of = top_z & even & (mw < wide - 1)
    passes = top_z & even & (mw > 0)
    hands = top_z & jnp.logical_not(even) & (mw < wide - 1)
    plain_rim = not_last & jnp.logical_not(hands)
    columns = max(wide // 2, 1)

    def relayed(w):
        return pairs - lax.div(max(pairs - KEEP, 0) * jnp.maximum(columns - 1 - lax.div(w, 2), 0), columns)

    @pl.when(hands)
    def _():
        greet(where_is(me + 1))

    @pl.when((mz == 0) & even & (mw > 0))
    def _():
        greet(where_is(me - 1))


    @pl.when(ahead_of)
    def _():
        greet({"wide": mw + 1, "narrow": 0})

    @pl.when(passes)
    def _():
        greet({"wide": mw, "narrow": 0})

    @pl.when((mz == 0) & (mw > 0))
    def _():
        greet({"wide": jnp.where(even, mw, mw - 1), "narrow": narrow - 1})

    @pl.when(mz == 0)
    def _():
        upin[...] = jnp.zeros_like(upin)

    @pl.when(top_z)
    def _():
        downin[...] = jnp.zeros_like(downin)

    downin[pl.ds(0, upin.shape[0] // wide), :] = jnp.zeros((upin.shape[0] // wide, LANES), F32)

    @pl.when(me == 0)
    def _():
        rimk[...] = jnp.zeros_like(rimk)
        rimv[...] = jnp.zeros_like(rimv)

    def cols(p):
        return pl.ds(pl.multiple_of(p * LANES, LANES), LANES)

    low = lax.broadcasted_iota(jnp.int32, (1, LANES), 1) < LANES // 2

    def piece(d):
        return pl.ds(pl.multiple_of(d * share, 8), share)

    packed = share == padded
    size = upin.shape[0] // wide

    def note(i):
        return pl.ds(pl.multiple_of(i * size, 8), size)

    def write(ref, i, tile):
        if not packed:
            ref[note(i), :] = tile
            return
        third = (padded - PLAIN) // 3
        rest = tile[PLAIN:padded, :]
        most = jnp.maximum(jnp.max(jnp.abs(rest), 0, keepdims=True), F32(1e-30))
        fine = F32(FINE) / most
        one = jnp.floor(rest[0:third, :] * fine + F32(0.5))
        two = jnp.floor(rest[third : 2 * third, :] * (fine * F32(0.5)) + F32(0.5))
        three = jnp.floor(rest[2 * third :, :] * fine + F32(0.5))
        high = jnp.floor(two * F32(1.0 / 256.0))
        at = i * size
        ref[pl.ds(pl.multiple_of(at, 8), PLAIN), :] = tile[0:PLAIN, :]
        ref[pl.ds(at + PLAIN - 1, 1), :] = most
        ref[pl.ds(pl.multiple_of(at + PLAIN, 8), third), :] = one * F32(256.0) + (high + F32(128.0))
        ref[pl.ds(pl.multiple_of(at + PLAIN + third, 8), third), :] = three * F32(256.0) + (two - high * F32(256.0))

    def read(ref, i):
        if not packed:
            return ref[note(i), :]
        third = (padded - PLAIN) // 3
        at = i * size
        plain = ref[pl.ds(pl.multiple_of(at, 8), PLAIN), :]
        left = ref[pl.ds(pl.multiple_of(at + PLAIN, 8), third), :]
        right = ref[pl.ds(pl.multiple_of(at + PLAIN + third, 8), third), :]
        step = plain[PLAIN - 1 : PLAIN, :] * F32(1.0 / FINE)
        one = jnp.floor(left * F32(1.0 / 256.0))
        three = jnp.floor(right * F32(1.0 / 256.0))
        two = (left - one * F32(256.0) - F32(128.0)) * F32(256.0) + (right - three * F32(256.0))
        return jnp.concatenate([plain, one * step, two * (step * F32(2.0)), three * step], 0)

    def first(k):
        d = other(k)
        return pltpu.make_async_remote_copy(
            src_ref=state.at[note(d), :], dst_ref=got.at[note(mw), :],
            send_sem=send1.at[k], recv_sem=recv1.at[k],
            device_id={"wide": d, "narrow": mz}, device_id_type=MESH,
        )

    def second(i, sender):
        return pltpu.make_async_remote_copy(
            src_ref=base.at[note(i), :], dst_ref=prior.at[note(mw), :],
            send_sem=send2.at[i], recv_sem=recv2.at[sender],
            device_id={"wide": i, "narrow": mz}, device_id_type=MESH,
        )

    def up(i):
        return pltpu.make_async_remote_copy(
            src_ref=upout.at[note(i), :], dst_ref=upin.at[note(i), :],
            send_sem=usend.at[i], recv_sem=urecv.at[i],
            device_id={"wide": mw, "narrow": lax.rem(mz + 1, narrow)}, device_id_type=MESH,
        )

    def down(i):
        return pltpu.make_async_remote_copy(
            src_ref=downout.at[note(i), :], dst_ref=downin.at[note(i), :],
            send_sem=dsend.at[i], recv_sem=drecv.at[i],
            device_id={"wide": mw, "narrow": lax.rem(mz + narrow - 1, narrow)}, device_id_type=MESH,
        )

    def rim(p, which):
        src, dst = ((wk_in, rimk), (val_in, rimv))[which]
        return pltpu.make_async_remote_copy(
            src_ref=src.at[:, cols(p)], dst_ref=dst.at[p],
            send_sem=rsend.at[which, p], recv_sem=rrecv.at[which, p],
            device_id=where_is(lax.rem(me + 1, n)), device_id_type=MESH,
        )

    def hand(p, which):
        src, dst = ((wk_in, farsk), (val_in, farsv))[which]
        return pltpu.make_async_remote_copy(
            src_ref=src.at[:, cols(p)], dst_ref=dst.at[p],
            send_sem=rsend.at[which, p], recv_sem=hrecv.at[which, p],
            device_id={"wide": other(1), "narrow": mz}, device_id_type=MESH,
        )

    def relay(p, which):
        src, dst = ((farsk, rimk), (farsv, rimv))[which]
        return pltpu.make_async_remote_copy(
            src_ref=src.at[p], dst_ref=dst.at[p],
            send_sem=psend.at[which, p], recv_sem=rrecv.at[which, p],
            device_id={"wide": mw, "narrow": 0}, device_id_type=MESH,
        )

    def rims(lo, hi):
        @pl.when(plain_rim)
        def _():
            @pl.loop(lo, hi)
            def _(p):
                rim(p, 0).start()
                rim(p, 1).start()

    def early(z):
        return jnp.minimum(jnp.where(z == narrow - 1, 0, EARLY + MORE * z), pairs)

    far = jnp.where(lax.rem(mw, 2) == 0, FAR, 0)

    def keys(p):
        x = fk[:, cols(lax.div(2 * p, per))]
        v = val[:, cols(p)]
        at = pl.multiple_of(p * padded, 8)
        parts = []
        norms = []
        for e in range(2):
            j = lax.rem(2 * p + e, per)
            a = nt(pick[0, j], x) + ccol[:, 0:1]
            b = nt(pick[1, j], x) + ccol[:, 1:2]
            k = (a * b * ccol[:, 2:3]).astype(BF16)
            kft[2 * p + e] = k
            parts.append(nn(k, v))
            norms.append(nt(jnp.ones((8, rows), BF16), k))
        own[pl.ds(at, padded), :] = jnp.where(low, parts[0], parts[1])
        for e in range(2):
            own[pl.ds(at + NORMS + 2 * e, 1), :] = norms[e][0:1, 0:LANES]
            own[pl.ds(at + NORMS + 2 * e + 1, 1), 0 : padded - LANES] = norms[e][0:1, LANES:padded]
        for e in range(chop):
            write(state, p * chop + e, own[piece(p * chop + e), :])

    def batch(g):
        return [lax.rem(lax.div(mw, chop) + 1 + g * GROUP + j, pairs) for j in range(GROUP)]

    def share_out(g):
        for p in batch(g):
            for e in range(chop):
                d = p * chop + e

                @pl.when(d != mw)
                def _():
                    first(lax.rem(d - mw + wide, wide)).start()

    for one in loads[:4]:
        one.wait()
    for p in batch(0):
        keys(p)
    pl.semaphore_wait(barrier, wide - 1 + (mz > 0) + jnp.logical_not(top_z) + ahead_of + passes + hands + ((mz == 0) & (mw > 0)) + ((mz == 0) & even & (mw > 0)))
    share_out(0)
    rims(0, early(mz))

    @pl.when(top_z)
    def _():
        rims(0, far)

    @pl.loop(1, pairs // GROUP)
    def _(g):
        for p in batch(g):
            keys(p)
        share_out(g)

    for one in loads[4:]:
        one.wait()

    r = lax.broadcasted_iota(jnp.int32, (rows, rows), 0)
    c = lax.broadcasted_iota(jnp.int32, (rows, rows), 1)
    causal = r >= c

    def intra(p):
        x = fq[:, cols(lax.div(2 * p, per))]
        v = val[:, cols(p)]
        nums = []
        dens = []
        for e in range(2):
            j = lax.rem(2 * p + e, per)
            a = nt(x, pick[0, j]) + crow[0:1, :]
            b = nt(x, pick[1, j]) + crow[1:2, :]
            q = (a * b * crow[2:3, :]).astype(BF16)
            qf[2 * p + e] = q
            s = jnp.where(causal, nn(q, kft[2 * p + e]), F32(0.0))
            dens.append(jnp.sum(s, -1, keepdims=True))
            nums.append(nn(s.astype(BF16), v))
        num[:, cols(p)] = jnp.where(low, nums[0], nums[1])
        den[:, cols(p)] = jnp.where(low, dens[0], dens[1])

    @pl.loop(0, AHEAD, unroll=2)
    def _(p):
        intra(p)

    @pl.loop(1, wide)
    def _(k):
        first(k).wait_recv()

    mine_tile = own[piece(mw), :]

    def add(d, total):
        scan[piece(d), :] = total
        total = total + jnp.where(d == mw, mine_tile, read(got, d))
        own[piece(d), :] = total
        return total

    lax.fori_loop(0, wide, add, jnp.zeros((share, LANES), F32))

    scale = BF16(1.0 / np.sqrt(LANES // 2))
    rim_ok = (c > r) & (me > 0)

    def attend(p):
        @pl.when(me > 0)
        def _():
            rim(p, 0).wait_recv()
            rim(p, 1).wait_recv()

        q = wq[:, cols(p)] * scale
        k = wk[:, cols(p)]
        v = val[:, cols(p)]
        rk = rimk[p]
        rv = rimv[p]
        outs = []
        for e in range(2):
            qe = jnp.where(low if e == 0 else ~low, q, jnp.zeros_like(q))
            s0 = jnp.where(rim_ok, nt(qe, rk), F32(-1e30))
            s1 = jnp.where(causal, nt(qe, k), F32(-1e30))
            m = jnp.maximum(jnp.max(s0, -1, keepdims=True), jnp.max(s1, -1, keepdims=True))
            e0 = jnp.exp(s0 - m)
            e1 = jnp.exp(s1 - m)
            inv = F32(1.0) / (jnp.sum(e0, -1, keepdims=True) + jnp.sum(e1, -1, keepdims=True))
            outs.append(nn((e0 * inv).astype(BF16), rv) + nn((e1 * inv).astype(BF16), v))
        return jnp.where(low, outs[0], outs[1])

    def part(p, e):
        q = wq[:, cols(p)] * scale
        return jnp.where(low if e == 0 else ~low, q, jnp.zeros_like(q))

    def begin(p):
        k = wk[:, cols(p)]
        for e in range(2):
            s1 = jnp.where(causal, nt(part(p, e), k), F32(-1e30))
            m = jnp.max(s1, -1, keepdims=True)
            e1 = jnp.exp(s1 - m)
            expo[2 * p + e] = e1
            peak[2 * p + e] = jnp.broadcast_to(m, (rows, LANES))
            mass[2 * p + e] = jnp.broadcast_to(jnp.sum(e1, -1, keepdims=True), (rows, LANES))

    def finish(p):
        @pl.when(me > 0)
        def _():
            rim(p, 0).wait_recv()
            rim(p, 1).wait_recv()

        v = val[:, cols(p)]
        rk = rimk[p]
        rv = rimv[p]
        outs = []
        for e in range(2):
            s0 = jnp.where(rim_ok, nt(part(p, e), rk), F32(-1e30))
            m1 = peak[2 * p + e]
            m = jnp.maximum(jnp.max(s0, -1, keepdims=True), m1)
            halves = [jnp.exp(s0[:, n : n + LANES] - m) for n in range(0, rows, LANES)]
            c1 = jnp.exp(m1 - m)
            inv = F32(1.0) / (jnp.sum(sum(halves), -1, keepdims=True) + mass[2 * p + e] * c1)
            c1 = c1 * inv
            w1 = jnp.concatenate([(expo[2 * p + e][:, n : n + LANES] * c1).astype(BF16) for n in range(0, rows, LANES)], 1)
            w0 = jnp.concatenate([(one * inv).astype(BF16) for one in halves], 1)
            outs.append(nn(w1, v) + nn(w0, rv))
        return jnp.where(low, outs[0], outs[1])

    lead = LAG * jnp.maximum(mz, narrow - 1 - mz)
    spent = wide - 1 + LAG * mz

    @pl.when(mz == 0)
    def _():
        @pl.loop(0, wide)
        def _(i):
            write(upout, i, own[piece(i), :])
            up(i).start()

        rims(early(mz), pairs)

    @pl.when(hands)
    def _():
        @pl.loop(0, relayed(mw))
        def _(p):
            hand(p, 0).start()
            hand(p, 1).start()


    left = 2 * (pairs - FAR)
    mixed = (wide - 1 - MIX) * BURST

    def either(make, q, act):
        for which in range(2):

            @pl.when(lax.rem(q, 2) == which)
            def _():
                act(make(lax.div(q, 2), which))

    def flow(q):
        @pl.when(ahead_of & (q < left))
        def _():
            either(rim, 2 * FAR + q, lambda copy: copy.start())

        @pl.when(passes & (q >= left) & (q < left + 2 * relayed(mw - 1)))
        def _():
            either(hand, q - left, lambda copy: copy.wait_recv())
            either(relay, q - left, lambda copy: copy.start())

    def slot(t):
        @pl.when(top_z & (t < wide - 1))
        def _():
            write(downout, t + 1, scan[piece(t + 1), :])
            down(t + 1).start()

            @pl.when(even & (t >= MIX))
            def _():
                for e in range(BURST):
                    flow((t - MIX) * BURST + e)

        @pl.when(top_z & even & (t >= PACE) & (lax.rem(t - PACE, STEP) == 0))
        def _():
            for e in range(RATE):
                flow(mixed + lax.div(t - PACE, STEP) * RATE + e)

        i = t - LAG * mz

        @pl.when((i >= 0) & (i < wide) & (mz > 0))
        def _():
            up(i).wait_recv()

            @pl.when(mz < narrow - 1)
            def _():
                write(upout, i, read(upin, i) + own[piece(i), :])
                up(i).start()

        j = t - LAG * (narrow - 1 - mz)

        @pl.when((j >= 1) & (j < wide) & (mz < narrow - 1))
        def _():
            down(j).wait_recv()

            @pl.when(mz > 0)
            def _():
                write(downout, j, read(downin, j) + scan[piece(j), :])
                down(j).start()

        o = t - lead

        @pl.when((o >= 0) & (o < wide))
        def _():
            tile = scan[piece(o), :] + read(upin, o) + read(downin, o)

            @pl.when(o == mw)
            def _():
                write(prior, o, tile)

            @pl.when(o != mw)
            def _():
                write(base, o, tile)
                second(o, mw).start()

        @pl.when((t == spent) & (mz > 0) & (mz < narrow - 1))
        def _():
            rims(early(mz), pairs)

    slots = wide + LAG * (narrow - 1)
    rest = pairs - AHEAD
    due = jnp.where(mz > 0, early(mz - 1), jnp.where(lax.rem(mw, 2) == 1, FAR, 0))
    done = jnp.minimum(due, slots - rest)

    @pl.loop(0, slots)
    def _(t):
        slot(t)

        @pl.when(t < rest)
        def _():
            intra(AHEAD + t)

        @pl.when((t >= rest) & (t - rest < done))
        def _():
            held[:, cols(t - rest)] = attend(t - rest)

        @pl.when((t - rest >= done) & (t - rest < pairs))
        def _():
            begin(t - rest)

    @pl.loop(jnp.maximum(slots - rest, done), pairs)
    def _(p):
        begin(p)

    @pl.when(top_z & even)
    def _():
        @pl.loop(mixed + max(0, -(-(slots - PACE) // STEP)) * RATE, left + 2 * pairs)
        def _(q):
            flow(q)

    soon = done + jnp.where((mz == 0) & even, FIRST, 0)

    @pl.loop(done, soon)
    def _(p):
        held[:, cols(p)] = finish(p)

    @pl.loop(1, wide)
    def _(k):
        second(other(k), other(k)).wait_recv()

    @pl.loop(0, pairs, unroll=4)
    def _(p):
        tile = jnp.concatenate([read(prior, p * chop + e) for e in range(chop)], 0)
        hi = tile.astype(BF16)
        mid = (tile - hi.astype(F32)).astype(BF16)
        crosses = []
        dens = []
        for e in range(2):
            qe = qf[2 * p + e]
            crosses.append(nn(qe, hi) + nn(qe, mid))
            at = NORMS + 2 * e
            z0 = tile[at : at + 1, :]
            z1 = tile[at + 1 : at + 2, 0 : padded - LANES]
            q32 = qe.astype(F32)
            dens.append(
                jnp.sum(q32[:, 0:LANES] * z0, -1, keepdims=True)
                + jnp.sum(q32[:, LANES:padded] * z1, -1, keepdims=True)
            )
        top = num[:, cols(p)] + jnp.where(low, crosses[0], crosses[1])
        bottom = den[:, cols(p)] + jnp.where(low, dens[0], dens[1])
        num[:, cols(p)] = top / bottom

    @pl.loop(0, soon)
    def _(p):
        out[:, cols(p)] = (num[:, cols(p)] + held[:, cols(p)]).astype(out.dtype)

    @pl.loop(1, wide)
    def _(k):
        first(k).wait_send()
        second(other(k), mw).wait_send()

    @pl.loop(0, wide)
    def _(i):
        @pl.when(mz < narrow - 1)
        def _():
            up(i).wait_send()

        @pl.when((mz > 0) & (i > 0))
        def _():
            down(i).wait_send()

    turn = jnp.clip(DIRECT, soon, pairs)

    @pl.loop(soon, turn)
    def _(p):
        out[:, cols(p)] = (num[:, cols(p)] + finish(p)).astype(out.dtype)

    @pl.when(hands)
    def _():
        @pl.loop(relayed(mw), pairs)
        def _(p):
            rim(p, 0).start()
            rim(p, 1).start()

    @pl.loop(turn, pairs)
    def _(p):
        out[:, cols(p)] = (num[:, cols(p)] + finish(p)).astype(out.dtype)

    @pl.when(not_last)
    def _():
        @pl.loop(0, pairs)
        def _(p):
            rim(p, 0).wait_send()
            rim(p, 1).wait_send()

    @pl.when(passes)
    def _():
        @pl.loop(0, relayed(mw - 1))
        def _(p):
            relay(p, 0).wait_send()
            relay(p, 1).wait_send()


def solution(mesh):
    wide, narrow = mesh.shape["wide"], mesh.shape["narrow"]

    def body(feat_queries, feat_keys, values, window_queries, window_keys):
        rows, channels = values.shape
        assert rows == WINDOW and channels == HEADS * LANES // 2
        padded, per, pick, extra = tables(feat_queries.shape[1] // HEADS)
        pairs = channels // LANES
        share = -(-pairs * padded // (8 * wide)) * 8
        whole = pltpu.VMEM((wide * share, LANES), F32)
        plain = layout(feat_queries.shape[1] // HEADS)[1]
        size = plain + (padded - plain) // 3 * 2 if share == padded else share
        notes = pltpu.VMEM((wide * size, LANES), F32)
        assert padded % share == 0
        ins = (
            feat_queries, feat_keys, values, window_queries, window_keys,
            jnp.asarray(pick, BF16), jnp.asarray(extra, F32), jnp.asarray(extra.T, F32),
        )
        ins = tuple(pltpu.with_memory_space_constraint(one, pltpu.HBM) for one in ins)
        return pl.pallas_call(
            functools.partial(kernel, (wide, narrow, padded, per, share)),
            out_shape=jax.ShapeDtypeStruct((rows, channels), BF16),
            in_specs=[pl.BlockSpec(memory_space=pltpu.HBM)] * 8,
            out_specs=pl.BlockSpec(memory_space=pltpu.VMEM),
            scratch_shapes=[
                *[pltpu.VMEM(one.shape, one.dtype) for one in ins],
                pltpu.VMEM((HEADS, rows, padded), BF16),
                pltpu.VMEM((HEADS, padded, rows), BF16),
                *[whole] * 2,
                *[notes] * 8,
                *[pltpu.VMEM((pairs, rows, LANES), BF16)] * 4,
                *[pltpu.VMEM((rows, channels), F32)] * 3,
                pltpu.VMEM((HEADS, rows, rows), F32),
                *[pltpu.VMEM((HEADS, rows, LANES), F32)] * 2,
                pltpu.SemaphoreType.DMA((8,)),
                *[pltpu.SemaphoreType.DMA((wide,))] * 8,
                *[pltpu.SemaphoreType.DMA((2, pairs))] * 4,
            ],
            compiler_params=pltpu.CompilerParams(
                collective_id=0, has_side_effects=True, vmem_limit_bytes=40 * 1024 * 1024
            ),
        )(*ins)

    spec = P(("wide", "narrow"), None)
    return jax.shard_map(
        body, mesh=mesh, in_specs=(spec,) * 5, out_specs=spec, check_vma=False
    )
```

```python
import functools

import jax
import jax.numpy as jnp
import numpy as np
from jax import lax
from jax.experimental import pallas as pl
from jax.experimental.pallas import tpu as pltpu
from jax.sharding import PartitionSpec as P

HEADS = 16
WINDOW = 256
LANES = 128
EARLY = 2
MORE = 1
AHEAD = 4
GROUP = 2
FAR = 5
PACE = 9
MIX = 0
STEP = 1
BURST = 1
RATE = 1
LAG = 2
FIRST = 3
DIRECT = 5
KEEP = 0
FINE = 65000.0
MESH = pl.DeviceIdType.MESH
F32 = jnp.float32
BF16 = jnp.bfloat16
NT = (((1,), (1,)), ((), ()))


def nt(a, b):
    return lax.dot_general(a, b, NT, preferred_element_type=F32)


def nn(a, b):
    return jnp.dot(a, b, preferred_element_type=F32)


def layout(width):
    norms = 1 + 2 * width
    return norms, -(-(norms + 5) // 8) * 8


def tables(width):
    norms, plain = layout(width)
    pairs = [(i, i) for i in range(width)] + [(i, j) for i in range(width) for j in range(i + 1, width)]
    padded = plain + -(-(len(pairs) - width) // 24) * 24
    per = LANES // width
    one = np.zeros((padded, width))
    two = np.zeros((padded, width))
    extra = np.zeros((8, padded))
    extra[0, 0] = 1.0
    extra[1, : 1 + width] = 1.0
    extra[2, 0] = 1.0
    extra[2, 1 : 1 + width] = 1.0 / width**0.25
    for i in range(width):
        one[1 + i, i] = 1.0
    for n, (i, j) in enumerate(pairs):
        at = 1 + width + n if n < width else plain + n - width
        one[at, i] = 1.0
        two[at, j] = 1.0
        extra[2, at] = 1.0 / np.sqrt(2.0 * width) if i == j else 1.0 / np.sqrt(1.0 * width)
    pick = np.zeros((2, per, padded, LANES))
    for j in range(per):
        pick[0, j, :, j * width : (j + 1) * width] = one
        pick[1, j, :, j * width : (j + 1) * width] = two
    return padded, per, pick, extra


def kernel(
    dims,
    fq_in, fk_in, val_in, wq_in, wk_in, pick_in, crow_in, ccol_in,
    out,
    fq, fk, val, wq, wk, pick, crow, ccol,
    qf, kft, own, scan, state, got, upin, upout, downin, downout, base, prior,
    rimk, rimv, farsk, farsv, num, den, held, expo, peak, mass,
    load, send1, recv1, send2, recv2, usend, urecv, dsend, drecv, rsend, rrecv, hrecv, psend,
):
    wide, narrow, padded, per, share = dims
    NORMS, PLAIN = layout(fq_in.shape[1] // HEADS)
    n = wide * narrow
    rows = val.shape[0]
    pairs = val.shape[1] // LANES
    chop = padded // share
    mw = lax.axis_index("wide")
    mz = lax.axis_index("narrow")
    me = mw * narrow + mz
    top_z = mz == narrow - 1
    not_last = me < n - 1

    ins = (fk_in, pick_in, ccol_in, val_in, fq_in, crow_in, wq_in, wk_in)
    mine = (fk, pick, ccol, val, fq, crow, wq, wk)
    loads = [pltpu.make_async_copy(i, m, load.at[j]) for j, (i, m) in enumerate(zip(ins, mine))]
    for one in loads:
        one.start()

    def where_is(d):
        return {"wide": lax.div(d, narrow), "narrow": lax.rem(d, narrow)}

    def other(k):
        return lax.rem(mw + k, wide)

    barrier = pltpu.get_barrier_semaphore()

    def greet(d):
        pl.semaphore_signal(barrier, inc=1, device_id=d, device_id_type=MESH)

    @pl.loop(1, wide)
    def _(k):
        greet({"wide": other(k), "narrow": mz})

    @pl.when(jnp.logical_not(top_z))
    def _():
        greet({"wide": mw, "narrow": mz + 1})

    @pl.when(mz > 0)
    def _():
        greet({"wide": mw, "narrow": mz - 1})

    even = lax.rem(mw, 2) == 0
    ahead_of = top_z & even & (mw < wide - 1)
    passes = top_z & even & (mw > 0)
    hands = top_z & jnp.logical_not(even) & (mw < wide - 1)
    plain_rim = not_last & jnp.logical_not(hands)
    columns = max(wide // 2, 1)

    def relayed(w):
        return pairs - lax.div(max(pairs - KEEP, 0) * jnp.maximum(columns - 1 - lax.div(w, 2), 0), columns)

    @pl.when(hands)
    def _():
        greet(where_is(me + 1))

    @pl.when((mz == 0) & even & (mw > 0))
    def _():
        greet(where_is(me - 1))


    @pl.when(ahead_of)
    def _():
        greet({"wide": mw + 1, "narrow": 0})

    @pl.when(passes)
    def _():
        greet({"wide": mw, "narrow": 0})

    @pl.when((mz == 0) & (mw > 0))
    def _():
        greet({"wide": jnp.where(even, mw, mw - 1), "narrow": narrow - 1})

    @pl.when(mz == 0)
    def _():
        upin[...] = jnp.zeros_like(upin)

    @pl.when(top_z)
    def _():
        downin[...] = jnp.zeros_like(downin)

    downin[pl.ds(0, upin.shape[0] // wide), :] = jnp.zeros((upin.shape[0] // wide, LANES), F32)

    @pl.when(me == 0)
    def _():
        rimk[...] = jnp.zeros_like(rimk)
        rimv[...] = jnp.zeros_like(rimv)

    def cols(p):
        return pl.ds(pl.multiple_of(p * LANES, LANES), LANES)

    low = lax.broadcasted_iota(jnp.int32, (1, LANES), 1) < LANES // 2

    def piece(d):
        return pl.ds(pl.multiple_of(d * share, 8), share)

    packed = share == padded
    size = upin.shape[0] // wide

    def note(i):
        return pl.ds(pl.multiple_of(i * size, 8), size)

    def write(ref, i, tile):
        if not packed:
            ref[note(i), :] = tile
            return
        third = (padded - PLAIN) // 3
        rest = tile[PLAIN:padded, :]
        most = jnp.maximum(jnp.max(jnp.abs(rest), 0, keepdims=True), F32(1e-30))
        fine = F32(FINE) / most
        one = jnp.floor(rest[0:third, :] * fine + F32(0.5))
        two = jnp.floor(rest[third : 2 * third, :] * (fine * F32(0.5)) + F32(0.5))
        three = jnp.floor(rest[2 * third :, :] * fine + F32(0.5))
        high = jnp.floor(two * F32(1.0 / 256.0))
        at = i * size
        ref[pl.ds(pl.multiple_of(at, 8), PLAIN), :] = tile[0:PLAIN, :]
        ref[pl.ds(at + PLAIN - 1, 1), :] = most
        ref[pl.ds(pl.multiple_of(at + PLAIN, 8), third), :] = one * F32(256.0) + (high + F32(128.0))
        ref[pl.ds(pl.multiple_of(at + PLAIN + third, 8), third), :] = three * F32(256.0) + (two - high * F32(256.0))

    def read(ref, i):
        if not packed:
            return ref[note(i), :]
        third = (padded - PLAIN) // 3
        at = i * size
        plain = ref[pl.ds(pl.multiple_of(at, 8), PLAIN), :]
        left = ref[pl.ds(pl.multiple_of(at + PLAIN, 8), third), :]
        right = ref[pl.ds(pl.multiple_of(at + PLAIN + third, 8), third), :]
        step = plain[PLAIN - 1 : PLAIN, :] * F32(1.0 / FINE)
        one = jnp.floor(left * F32(1.0 / 256.0))
        three = jnp.floor(right * F32(1.0 / 256.0))
        two = (left - one * F32(256.0) - F32(128.0)) * F32(256.0) + (right - three * F32(256.0))
        return jnp.concatenate([plain, one * step, two * (step * F32(2.0)), three * step], 0)

    def first(k):
        d = other(k)
        return pltpu.make_async_remote_copy(
            src_ref=state.at[note(d), :], dst_ref=got.at[note(mw), :],
            send_sem=send1.at[k], recv_sem=recv1.at[k],
            device_id={"wide": d, "narrow": mz}, device_id_type=MESH,
        )

    def second(i, sender):
        return pltpu.make_async_remote_copy(
            src_ref=base.at[note(i), :], dst_ref=prior.at[note(mw), :],
            send_sem=send2.at[i], recv_sem=recv2.at[sender],
            device_id={"wide": i, "narrow": mz}, device_id_type=MESH,
        )

    def up(i):
        return pltpu.make_async_remote_copy(
            src_ref=upout.at[note(i), :], dst_ref=upin.at[note(i), :],
            send_sem=usend.at[i], recv_sem=urecv.at[i],
            device_id={"wide": mw, "narrow": lax.rem(mz + 1, narrow)}, device_id_type=MESH,
        )

    def down(i):
        return pltpu.make_async_remote_copy(
            src_ref=downout.at[note(i), :], dst_ref=downin.at[note(i), :],
            send_sem=dsend.at[i], recv_sem=drecv.at[i],
            device_id={"wide": mw, "narrow": lax.rem(mz + narrow - 1, narrow)}, device_id_type=MESH,
        )

    def rim(p, which):
        src, dst = ((wk_in, rimk), (val_in, rimv))[which]
        return pltpu.make_async_remote_copy(
            src_ref=src.at[:, cols(p)], dst_ref=dst.at[p],
            send_sem=rsend.at[which, p], recv_sem=rrecv.at[which, p],
            device_id=where_is(lax.rem(me + 1, n)), device_id_type=MESH,
        )

    def hand(p, which):
        src, dst = ((wk_in, farsk), (val_in, farsv))[which]
        return pltpu.make_async_remote_copy(
            src_ref=src.at[:, cols(p)], dst_ref=dst.at[p],
            send_sem=rsend.at[which, p], recv_sem=hrecv.at[which, p],
            device_id={"wide": other(1), "narrow": mz}, device_id_type=MESH,
        )

    def relay(p, which):
        src, dst = ((farsk, rimk), (farsv, rimv))[which]
        return pltpu.make_async_remote_copy(
            src_ref=src.at[p], dst_ref=dst.at[p],
            send_sem=psend.at[which, p], recv_sem=rrecv.at[which, p],
            device_id={"wide": mw, "narrow": 0}, device_id_type=MESH,
        )

    def rims(lo, hi):
        @pl.when(plain_rim)
        def _():
            @pl.loop(lo, hi)
            def _(p):
                rim(p, 0).start()
                rim(p, 1).start()

    def early(z):
        return jnp.minimum(jnp.where(z == narrow - 1, 0, EARLY + MORE * z), pairs)

    far = jnp.where(lax.rem(mw, 2) == 0, FAR, 0)

    def keys(p):
        x = fk[:, cols(lax.div(2 * p, per))]
        v = val[:, cols(p)]
        at = pl.multiple_of(p * padded, 8)
        parts = []
        norms = []
        for e in range(2):
            j = lax.rem(2 * p + e, per)
            a = nt(pick[0, j], x) + ccol[:, 0:1]
            b = nt(pick[1, j], x) + ccol[:, 1:2]
            k = (a * b * ccol[:, 2:3]).astype(BF16)
            kft[2 * p + e] = k
            parts.append(nn(k, v))
            norms.append(nt(jnp.ones((8, rows), BF16), k))
        own[pl.ds(at, padded), :] = jnp.where(low, parts[0], parts[1])
        for e in range(2):
            own[pl.ds(at + NORMS + 2 * e, 1), :] = norms[e][0:1, 0:LANES]
            own[pl.ds(at + NORMS + 2 * e + 1, 1), 0 : padded - LANES] = norms[e][0:1, LANES:padded]
        for e in range(chop):
            write(state, p * chop + e, own[piece(p * chop + e), :])

    def batch(g):
        return [lax.rem(lax.div(mw, chop) + 1 + g * GROUP + j, pairs) for j in range(GROUP)]

    def share_out(g):
        for p in batch(g):
            for e in range(chop):
                d = p * chop + e

                @pl.when(d != mw)
                def _():
                    first(lax.rem(d - mw + wide, wide)).start()

    for one in loads[:4]:
        one.wait()
    for p in batch(0):
        keys(p)
    pl.semaphore_wait(barrier, wide - 1 + (mz > 0) + jnp.logical_not(top_z) + ahead_of + passes + hands + ((mz == 0) & (mw > 0)) + ((mz == 0) & even & (mw > 0)))
    share_out(0)
    rims(0, early(mz))

    @pl.when(top_z)
    def _():
        rims(0, far)

    @pl.loop(1, pairs // GROUP)
    def _(g):
        for p in batch(g):
            keys(p)
        share_out(g)

    for one in loads[4:]:
        one.wait()

    r = lax.broadcasted_iota(jnp.int32, (rows, rows), 0)
    c = lax.broadcasted_iota(jnp.int32, (rows, rows), 1)
    causal = r >= c

    def intra(p):
        x = fq[:, cols(lax.div(2 * p, per))]
        v = val[:, cols(p)]
        nums = []
        dens = []
        for e in range(2):
            j = lax.rem(2 * p + e, per)
            a = nt(x, pick[0, j]) + crow[0:1, :]
            b = nt(x, pick[1, j]) + crow[1:2, :]
            q = (a * b * crow[2:3, :]).astype(BF16)
            qf[2 * p + e] = q
            s = jnp.where(causal, nn(q, kft[2 * p + e]), F32(0.0))
            dens.append(jnp.sum(s, -1, keepdims=True))
            nums.append(nn(s.astype(BF16), v))
        num[:, cols(p)] = jnp.where(low, nums[0], nums[1])
        den[:, cols(p)] = jnp.where(low, dens[0], dens[1])

    @pl.loop(0, AHEAD, unroll=2)
    def _(p):
        intra(p)

    @pl.loop(1, wide)
    def _(k):
        first(k).wait_recv()

    mine_tile = own[piece(mw), :]

    def add(d, total):
        scan[piece(d), :] = total
        total = total + jnp.where(d == mw, mine_tile, read(got, d))
        own[piece(d), :] = total
        return total

    lax.fori_loop(0, wide, add, jnp.zeros((share, LANES), F32))

    scale = BF16(1.0 / np.sqrt(LANES // 2))
    rim_ok = (c > r) & (me > 0)

    def attend(p):
        @pl.when(me > 0)
        def _():
            rim(p, 0).wait_recv()
            rim(p, 1).wait_recv()

        q = wq[:, cols(p)] * scale
        k = wk[:, cols(p)]
        v = val[:, cols(p)]
        rk = rimk[p]
        rv = rimv[p]
        outs = []
        for e in range(2):
            qe = jnp.where(low if e == 0 else ~low, q, jnp.zeros_like(q))
            s0 = jnp.where(rim_ok, nt(qe, rk), F32(-1e30))
            s1 = jnp.where(causal, nt(qe, k), F32(-1e30))
            m = jnp.maximum(jnp.max(s0, -1, keepdims=True), jnp.max(s1, -1, keepdims=True))
            e0 = jnp.exp(s0 - m)
            e1 = jnp.exp(s1 - m)
            inv = F32(1.0) / (jnp.sum(e0, -1, keepdims=True) + jnp.sum(e1, -1, keepdims=True))
            outs.append(nn((e0 * inv).astype(BF16), rv) + nn((e1 * inv).astype(BF16), v))
        return jnp.where(low, outs[0], outs[1])

    def part(p, e):
        q = wq[:, cols(p)] * scale
        return jnp.where(low if e == 0 else ~low, q, jnp.zeros_like(q))

    def begin(p):
        k = wk[:, cols(p)]
        for e in range(2):
            s1 = jnp.where(causal, nt(part(p, e), k), F32(-1e30))
            m = jnp.max(s1, -1, keepdims=True)
            e1 = jnp.exp(s1 - m)
            expo[2 * p + e] = e1
            peak[2 * p + e] = jnp.broadcast_to(m, (rows, LANES))
            mass[2 * p + e] = jnp.broadcast_to(jnp.sum(e1, -1, keepdims=True), (rows, LANES))

    def finish(p):
        @pl.when(me > 0)
        def _():
            rim(p, 0).wait_recv()
            rim(p, 1).wait_recv()

        v = val[:, cols(p)]
        rk = rimk[p]
        rv = rimv[p]
        outs = []
        for e in range(2):
            s0 = jnp.where(rim_ok, nt(part(p, e), rk), F32(-1e30))
            m1 = peak[2 * p + e]
            m = jnp.maximum(jnp.max(s0, -1, keepdims=True), m1)
            halves = [jnp.exp(s0[:, n : n + LANES] - m) for n in range(0, rows, LANES)]
            c1 = jnp.exp(m1 - m)
            inv = F32(1.0) / (jnp.sum(sum(halves), -1, keepdims=True) + mass[2 * p + e] * c1)
            c1 = c1 * inv
            w1 = jnp.concatenate([(expo[2 * p + e][:, n : n + LANES] * c1).astype(BF16) for n in range(0, rows, LANES)], 1)
            w0 = jnp.concatenate([(one * inv).astype(BF16) for one in halves], 1)
            outs.append(nn(w1, v) + nn(w0, rv))
        return jnp.where(low, outs[0], outs[1])

    lead = LAG * jnp.maximum(mz, narrow - 1 - mz)
    spent = wide - 1 + LAG * mz

    @pl.when(mz == 0)
    def _():
        @pl.loop(0, wide)
        def _(i):
            write(upout, i, own[piece(i), :])
            up(i).start()

        rims(early(mz), pairs)

    @pl.when(hands)
    def _():
        @pl.loop(0, relayed(mw))
        def _(p):
            hand(p, 0).start()
            hand(p, 1).start()


    left = 2 * (pairs - FAR)
    mixed = (wide - 1 - MIX) * BURST

    def either(make, q, act):
        for which in range(2):

            @pl.when(lax.rem(q, 2) == which)
            def _():
                act(make(lax.div(q, 2), which))

    def flow(q):
        @pl.when(ahead_of & (q < left))
        def _():
            either(rim, 2 * FAR + q, lambda copy: copy.start())

        @pl.when(passes & (q >= left) & (q < left + 2 * relayed(mw - 1)))
        def _():
            either(hand, q - left, lambda copy: copy.wait_recv())
            either(relay, q - left, lambda copy: copy.start())

    def slot(t):
        @pl.when(top_z & (t < wide - 1))
        def _():
            write(downout, t + 1, scan[piece(t + 1), :])
            down(t + 1).start()

            @pl.when(even & (t >= MIX))
            def _():
                for e in range(BURST):
                    flow((t - MIX) * BURST + e)

        @pl.when(top_z & even & (t >= PACE) & (lax.rem(t - PACE, STEP) == 0))
        def _():
            for e in range(RATE):
                flow(mixed + lax.div(t - PACE, STEP) * RATE + e)

        i = t - LAG * mz

        @pl.when((i >= 0) & (i < wide) & (mz > 0))
        def _():
            up(i).wait_recv()

            @pl.when(mz < narrow - 1)
            def _():
                write(upout, i, read(upin, i) + own[piece(i), :])
                up(i).start()

        j = t - LAG * (narrow - 1 - mz)

        @pl.when((j >= 1) & (j < wide) & (mz < narrow - 1))
        def _():
            down(j).wait_recv()

            @pl.when(mz > 0)
            def _():
                write(downout, j, read(downin, j) + scan[piece(j), :])
                down(j).start()

        o = t - lead

        @pl.when((o >= 0) & (o < wide))
        def _():
            tile = scan[piece(o), :] + read(upin, o) + read(downin, o)

            @pl.when(o == mw)
            def _():
                write(prior, o, tile)

            @pl.when(o != mw)
            def _():
                write(base, o, tile)
                second(o, mw).start()

        @pl.when((t == spent) & (mz > 0) & (mz < narrow - 1))
        def _():
            rims(early(mz), pairs)

    slots = wide + LAG * (narrow - 1)
    rest = pairs - AHEAD
    due = jnp.where(mz > 0, early(mz - 1), jnp.where(lax.rem(mw, 2) == 1, FAR, 0))
    done = jnp.minimum(due, slots - rest)

    @pl.loop(0, slots)
    def _(t):
        slot(t)

        @pl.when(t < rest)
        def _():
            intra(AHEAD + t)

        @pl.when((t >= rest) & (t - rest < done))
        def _():
            held[:, cols(t - rest)] = attend(t - rest)

        @pl.when((t - rest >= done) & (t - rest < pairs))
        def _():
            begin(t - rest)

    @pl.loop(jnp.maximum(slots - rest, done), pairs)
    def _(p):
        begin(p)

    @pl.when(top_z & even)
    def _():
        @pl.loop(mixed + max(0, -(-(slots - PACE) // STEP)) * RATE, left + 2 * pairs)
        def _(q):
            flow(q)

    soon = done + jnp.where((mz == 0) & even, FIRST, 0)

    @pl.loop(done, soon)
    def _(p):
        held[:, cols(p)] = finish(p)

    @pl.loop(1, wide)
    def _(k):
        second(other(k), other(k)).wait_recv()

    @pl.loop(0, pairs, unroll=4)
    def _(p):
        tile = jnp.concatenate([read(prior, p * chop + e) for e in range(chop)], 0)
        hi = tile.astype(BF16)
        mid = (tile - hi.astype(F32)).astype(BF16)
        crosses = []
        dens = []
        for e in range(2):
            qe = qf[2 * p + e]
            crosses.append(nn(qe, hi) + nn(qe, mid))
            at = NORMS + 2 * e
            z0 = tile[at : at + 1, :]
            z1 = tile[at + 1 : at + 2, 0 : padded - LANES]
            q32 = qe.astype(F32)
            dens.append(
                jnp.sum(q32[:, 0:LANES] * z0, -1, keepdims=True)
                + jnp.sum(q32[:, LANES:padded] * z1, -1, keepdims=True)
            )
        top = num[:, cols(p)] + jnp.where(low, crosses[0], crosses[1])
        bottom = den[:, cols(p)] + jnp.where(low, dens[0], dens[1])
        num[:, cols(p)] = top / bottom

    @pl.loop(0, soon)
    def _(p):
        out[:, cols(p)] = (num[:, cols(p)] + held[:, cols(p)]).astype(out.dtype)

    @pl.loop(1, wide)
    def _(k):
        first(k).wait_send()
        second(other(k), mw).wait_send()

    @pl.loop(0, wide)
    def _(i):
        @pl.when(mz < narrow - 1)
        def _():
            up(i).wait_send()

        @pl.when((mz > 0) & (i > 0))
        def _():
            down(i).wait_send()

    @pl.when(not_last & (mz == 0))
    def _():
        @pl.loop(0, pairs)
        def _(p):
            rim(p, 0).wait_send()
            rim(p, 1).wait_send()

    turn = jnp.clip(DIRECT, soon, pairs)

    @pl.loop(soon, turn)
    def _(p):
        out[:, cols(p)] = (num[:, cols(p)] + finish(p)).astype(out.dtype)

    @pl.when(hands)
    def _():
        @pl.loop(relayed(mw), pairs)
        def _(p):
            rim(p, 0).start()
            rim(p, 1).start()

    @pl.loop(turn, pairs)
    def _(p):
        out[:, cols(p)] = (num[:, cols(p)] + finish(p)).astype(out.dtype)

    @pl.when(not_last & (mz > 0))
    def _():
        @pl.loop(0, pairs)
        def _(p):
            rim(p, 0).wait_send()
            rim(p, 1).wait_send()

    @pl.when(passes)
    def _():
        @pl.loop(0, relayed(mw - 1))
        def _(p):
            relay(p, 0).wait_send()
            relay(p, 1).wait_send()


def solution(mesh):
    wide, narrow = mesh.shape["wide"], mesh.shape["narrow"]

    def body(feat_queries, feat_keys, values, window_queries, window_keys):
        rows, channels = values.shape
        assert rows == WINDOW and channels == HEADS * LANES // 2
        padded, per, pick, extra = tables(feat_queries.shape[1] // HEADS)
        pairs = channels // LANES
        share = -(-pairs * padded // (8 * wide)) * 8
        whole = pltpu.VMEM((wide * share, LANES), F32)
        plain = layout(feat_queries.shape[1] // HEADS)[1]
        size = plain + (padded - plain) // 3 * 2 if share == padded else share
        notes = pltpu.VMEM((wide * size, LANES), F32)
        assert padded % share == 0
        ins = (
            feat_queries, feat_keys, values, window_queries, window_keys,
            jnp.asarray(pick, BF16), jnp.asarray(extra, F32), jnp.asarray(extra.T, F32),
        )
        ins = tuple(pltpu.with_memory_space_constraint(one, pltpu.HBM) for one in ins)
        return pl.pallas_call(
            functools.partial(kernel, (wide, narrow, padded, per, share)),
            out_shape=jax.ShapeDtypeStruct((rows, channels), BF16),
            in_specs=[pl.BlockSpec(memory_space=pltpu.HBM)] * 8,
            out_specs=pl.BlockSpec(memory_space=pltpu.VMEM),
            scratch_shapes=[
                *[pltpu.VMEM(one.shape, one.dtype) for one in ins],
                pltpu.VMEM((HEADS, rows, padded), BF16),
                pltpu.VMEM((HEADS, padded, rows), BF16),
                *[whole] * 2,
                *[notes] * 8,
                *[pltpu.VMEM((pairs, rows, LANES), BF16)] * 4,
                *[pltpu.VMEM((rows, channels), F32)] * 3,
                pltpu.VMEM((HEADS, rows, rows), F32),
                *[pltpu.VMEM((HEADS, rows, LANES), F32)] * 2,
                pltpu.SemaphoreType.DMA((8,)),
                *[pltpu.SemaphoreType.DMA((wide,))] * 8,
                *[pltpu.SemaphoreType.DMA((2, pairs))] * 4,
            ],
            compiler_params=pltpu.CompilerParams(
                collective_id=0, has_side_effects=True, vmem_limit_bytes=40 * 1024 * 1024
            ),
        )(*ins)

    spec = P(("wide", "narrow"), None)
    return jax.shard_map(
        body, mesh=mesh, in_specs=(spec,) * 5, out_specs=spec, check_vma=False
    )
```
